256 devices in a mesh: dp: 256 (over z, y, x, core).
Axes of the slice: x: 4, y: 4, z: 8, core: 2. Of those that a mesh axis runs over, the one named last changes fastest.
Arguments:
- user_x: float32 [32768, 256], P('dp')
- item_x: float32 [32768, 256], P('dp')
- item_id: int32 [32768], P('dp')
- log_q: float32 [32768], P('dp')
- user_w1: float32 [256, 384], replicated
- user_w2: float32 [384, 384], replicated
- user_w3: float32 [384, 128], replicated
- item_w1: float32 [256, 384], replicated
- item_w2: float32 [384, 384], replicated
- item_w3: float32 [384, 128], replicated
Outputs:
- output 1: float32 [], replicated
- output 2: float32 [256, 384], replicated
- output 3: float32 [384, 384], replicated
- output 4: float32 [384, 128], replicated
- output 5: float32 [256, 384], replicated
- output 6: float32 [384, 384], replicated
- output 7: float32 [384, 128], replicated
All inputs are finite; a program needn't handle non-finite values.
Results may differ from the reference program's by a relative error of at most 0.00200594.
Values are sent between devices in bfloat16 or wider.
A program may use at most 768 MiB of HBM per device.

```python
import jax
import jax.numpy as jnp
from jax import lax

ROWS_DEV = 128
GROUP_SIZE = 256
IN_WIDTH = 256
HIDDEN_A = 384
HIDDEN_B = 384
EMBED_DIM = 128

BATCH = ROWS_DEV * GROUP_SIZE
ID_RANGE = max(BATCH // 64, 2)
TEMPERATURE = 0.05
INV_TEMP = 1.0 / TEMPERATURE
NORM_EPS = 1e-6


def id_features(key, item_id):
    def one_row(one_id):
        return jax.random.normal(jax.random.fold_in(key, one_id), (IN_WIDTH,), jnp.float32)
    return jax.vmap(one_row)(item_id)


def setup_inputs(seed: int = 0) -> dict:
    keys = jax.random.split(jax.random.key(seed), 12)
    shapes = ((IN_WIDTH, HIDDEN_A), (HIDDEN_A, HIDDEN_B), (HIDDEN_B, EMBED_DIM))
    gains = (2.0, 2.0, 1.0)
    user_ws = []
    item_ws = []
    for layer in range(3):
        scale = (gains[layer] / shapes[layer][0]) ** 0.5
        base = jax.random.normal(keys[layer], shapes[layer], jnp.float32)
        other = jax.random.normal(keys[layer + 3], shapes[layer], jnp.float32)
        user_ws.append(base * scale)
        item_ws.append((0.95 * base + 0.31 * other) * scale)
    item_id = jax.random.randint(keys[6], (BATCH,), 0, ID_RANGE, dtype=jnp.int32)
    item_x = 0.97 * id_features(keys[7], item_id) + 0.243 * jax.random.normal(keys[8], (BATCH, IN_WIDTH), jnp.float32)
    user_x = 0.95 * item_x + 0.31 * jax.random.normal(keys[9], (BATCH, IN_WIDTH), jnp.float32)
    log_q = jax.random.uniform(keys[10], (BATCH,), jnp.float32, -12.0, -6.0)
    return {'user_x': user_x, 'item_x': item_x, 'item_id': item_id, 'log_q': log_q,
            'user_w1': user_ws[0], 'user_w2': user_ws[1], 'user_w3': user_ws[2],
            'item_w1': item_ws[0], 'item_w2': item_ws[1], 'item_w3': item_ws[2]}


def tower_forward(inputs, w_one, w_two, w_three):
    x_half = inputs.astype(jnp.bfloat16)
    pre_one = jnp.dot(x_half, w_one.astype(jnp.bfloat16), preferred_element_type=jnp.float32)
    act_one = jnp.maximum(pre_one, 0.0).astype(jnp.bfloat16)
    pre_two = jnp.dot(act_one, w_two.astype(jnp.bfloat16), preferred_element_type=jnp.float32)
    act_two = jnp.maximum(pre_two, 0.0).astype(jnp.bfloat16)
    raw_out = jnp.dot(act_two, w_three.astype(jnp.bfloat16), preferred_element_type=jnp.float32)
    inv_norm = lax.rsqrt(jnp.sum(raw_out * raw_out, axis=1, keepdims=True) + NORM_EPS)
    return (x_half, pre_one, act_one, pre_two, act_two, raw_out * inv_norm, inv_norm)


def tower_grads(inputs, w_one, w_two, w_three, grad_unit):
    x_half, pre_one, act_one, pre_two, act_two, unit_out, inv_norm = tower_forward(inputs, w_one, w_two, w_three)
    grad_raw = inv_norm * (grad_unit - unit_out * jnp.sum(unit_out * grad_unit, axis=1, keepdims=True))
    grad_raw_h = grad_raw.astype(jnp.bfloat16)
    grad_three = jnp.dot(act_two.T, grad_raw_h, preferred_element_type=jnp.float32)
    grad_act_two = jnp.dot(grad_raw_h, w_three.astype(jnp.bfloat16).T, preferred_element_type=jnp.float32)
    grad_pre_two = jnp.where(pre_two > 0.0, grad_act_two, 0.0).astype(jnp.bfloat16)
    grad_two = jnp.dot(act_one.T, grad_pre_two, preferred_element_type=jnp.float32)
    grad_act_one = jnp.dot(grad_pre_two, w_two.astype(jnp.bfloat16).T, preferred_element_type=jnp.float32)
    grad_pre_one = jnp.where(pre_one > 0.0, grad_act_one, 0.0).astype(jnp.bfloat16)
    grad_one = jnp.dot(x_half.T, grad_pre_one, preferred_element_type=jnp.float32)
    return (grad_one, grad_two, grad_three)


def accumulate_grads(x_shards, grad_shards, w_one, w_two, w_three):
    def grad_step(carry, shard):
        step_grads = tower_grads(shard[0], w_one, w_two, w_three, shard[1])
        return tuple(total + part for total, part in zip(carry, step_grads)), None
    zeros = (jnp.zeros(w_one.shape, jnp.float32), jnp.zeros(w_two.shape, jnp.float32), jnp.zeros(w_three.shape, jnp.float32))
    return lax.scan(grad_step, zeros, (x_shards, grad_shards))[0]


def reference(user_x, item_x, item_id, log_q, user_w1, user_w2, user_w3, item_w1, item_w2, item_w3):
    user_shards = user_x.reshape(GROUP_SIZE, ROWS_DEV, IN_WIDTH)
    item_shards = item_x.reshape(GROUP_SIZE, ROWS_DEV, IN_WIDTH)
    user_half = lax.map(lambda rows_in: tower_forward(rows_in, user_w1, user_w2, user_w3)[5], user_shards).astype(jnp.bfloat16)
    item_half = lax.map(lambda rows_in: tower_forward(rows_in, item_w1, item_w2, item_w3)[5], item_shards).astype(jnp.bfloat16)
    item_all = item_half.reshape(BATCH, EMBED_DIM)
    cand_pos = jnp.arange(BATCH)

    def query_step(grad_item_sum, shard):
        user_rows, item_rows, id_rows, logq_rows, shard_index = shard
        query_pos = shard_index * ROWS_DEV + jnp.arange(ROWS_DEV)
        raw = jnp.dot(user_rows, item_all.T, preferred_element_type=jnp.float32) * INV_TEMP - log_q[None, :]
        is_self = query_pos[:, None] == cand_pos[None, :]
        dropped = jnp.logical_and(id_rows[:, None] == item_id[None, :], jnp.logical_not(is_self))
        scores = jnp.where(dropped, -jnp.inf, raw)
        row_max = jnp.max(scores, axis=1, keepdims=True)
        exp_scores = jnp.exp(scores - row_max)
        row_total = jnp.sum(exp_scores, axis=1, keepdims=True)
        log_norm = row_max[:, 0] + jnp.log(row_total[:, 0])
        pos_score = jnp.sum(user_rows.astype(jnp.float32) * item_rows.astype(jnp.float32), axis=1) * INV_TEMP - logq_rows
        softmax_rows = exp_scores / row_total
        grad_scores = (jnp.where(is_self, softmax_rows - 1.0, softmax_rows) / BATCH).astype(jnp.bfloat16)
        grad_user = jnp.dot(grad_scores, item_all, preferred_element_type=jnp.float32) * INV_TEMP
        item_part = jnp.dot(grad_scores.T, user_rows, preferred_element_type=jnp.float32) * INV_TEMP
        return grad_item_sum + item_part, (jnp.sum(log_norm - pos_score), grad_user)

    grad_item, step_out = lax.scan(query_step, jnp.zeros((BATCH, EMBED_DIM), jnp.float32),
                                   (user_half, item_half, item_id.reshape(GROUP_SIZE, ROWS_DEV),
                                    log_q.reshape(GROUP_SIZE, ROWS_DEV), jnp.arange(GROUP_SIZE)))
    loss_parts, grad_user = step_out
    user_grads = accumulate_grads(user_shards, grad_user, user_w1, user_w2, user_w3)
    item_grads = accumulate_grads(item_shards, grad_item.reshape(GROUP_SIZE, ROWS_DEV, EMBED_DIM), item_w1, item_w2, item_w3)
    loss = jnp.sum(loss_parts) / BATCH
    return (loss, user_grads[0], user_grads[1], user_grads[2], item_grads[0], item_grads[1], item_grads[2])
```

```python
import functools
import math

import jax
import jax.numpy as jnp
from jax import lax
from jax.experimental import pallas as pl
from jax.experimental.pallas import tpu as pltpu
from jax.sharding import PartitionSpec as P

F32, BF16, I32 = jnp.float32, jnp.bfloat16, jnp.int32
MESH = pl.DeviceIdType.MESH

GRID = {256: (8, 4, 4)}
UNITS_PER_Z = None

L, SUB = 128, 8
PAIR = range(2)
USER, ITEM = PAIR
W_IN, W_A, W_B = 256, 384, 384
DUO = 2 * L
MAX_GROUPS = 32
TEMP = 0.05
INV_TEMP = 1.0 / TEMP
EXP_SCALE = INV_TEMP * math.log2(math.e)
NORM_EPS = 1e-6
LOW = -3.0e38
ROWS_1, ROWS_2, ROWS_3 = W_IN * W_A // L, W_A * W_B // L, W_B
AT_2, AT_3 = ROWS_1, ROWS_1 + ROWS_2
GRAD_ROWS = AT_3 + ROWS_3
HALF_ROWS = GRAD_ROWS // 2
COLS = W_A // L
X_AT, H1_AT, H2_AT, ACT_ROWS = 0, W_IN, W_IN + W_A, W_IN + W_A + W_B
VMEM_BYTES, LAYOUT_BYTES = 56 << 20, 1 << 20
LAG_V, LAG_DV = 4, 5
NN = (((1,), (0,)), ((), ()))
NT = (((1,), (1,)), ((), ()))


def _dot(a, b, dims=NN):
    return lax.dot_general(a, b, dims, preferred_element_type=F32)


def _near(k):
    return k + k // 2 - 2 * (k // 3)


def _lanes(j, n=1):
    return slice(j * L, (j + n) * L)


def _at(start, size):
    return pl.ds(pl.multiple_of(start, SUB), size)


def _peers(n):
    return range(1, n)


def _iota(shape, dim):
    return lax.broadcasted_iota(I32, shape, dim)


class _Marks:
    def __init__(self):
        self.scope = None

    def __call__(self, name=None):
        if self.scope is not None:
            self.scope.__exit__(None, None, None)
        self.scope = jax.named_scope(name) if name else None
        if name:
            self.scope.__enter__()


class _Plan:
    def __init__(self, n):
        nz, ny, nx = self.nz, self.ny, self.nx = GRID[n]
        self.plane = nx * ny
        self.batch = n * L
        self.queries = nz * L
        self.c2 = HALF_ROWS // self.plane
        self.n1, self.n2 = (nx, ny), (ny, nx)
        self.c1 = tuple(HALF_ROWS // m for m in self.n1)
        self.w = (UNITS_PER_Z or self.c2 // SUB // nz) * SUB
        self.rest = self.c2 - nz * self.w
        self.tail = 2 * self.rest + SUB
        self.offsets = [(_near(k // nx), _near(k % nx)) for k in range(self.plane)]
        self.zorder = sorted(range(nz), key=lambda d: -min(d, nz - d))
        self.own = self.zorder.index(0)

    def slot(self, dy, dx):
        return self.offsets.index((dy % self.ny, dx % self.nx))

    def tile(self, dz):
        return self.zorder.index(dz % self.nz)


def _scratch(p):
    npl, nz, nq = p.plane, p.nz, p.queries
    vm, dma = pltpu.VMEM, pltpu.SemaphoreType.DMA
    groups, most = 2 * npl, max(p.n1)
    nrx = max(groups, 2 * nz)
    a1 = p.c1[0] + SUB
    return dict(
        xs=vm((2, L, W_IN), F32),
        wf1=vm((2, W_IN, W_A), F32),
        wf2=vm((2, W_A, W_B), F32),
        wf3=vm((2, W_B, L), F32),
        w2=vm((2, W_A, W_B), BF16),
        w3=vm((2, W_B, L), BF16),
        acts=vm((2, ACT_ROWS, DUO), BF16),
        hid=vm((2, DUO, W_A + W_B), BF16),
        unit=vm((2, DUO, DUO), F32),
        idb=vm((groups, 1, L), I32),
        lqb=vm((groups, 1, L), F32),
        idq=vm((nz, 1, L), I32),
        idk=vm((MAX_GROUPS, L), I32),
        lqk=vm((MAX_GROUPS, L), F32),
        idc=vm((npl, DUO, L), I32),
        vaug=vm((npl, DUO, DUO), BF16),
        vt=vm((npl, L, DUO), BF16),
        uall=vm((nq, L), BF16),
        ut=vm((DUO, nq), BF16),
        tb=vm((npl, DUO, nq), F32),
        ls=vm((SUB, nq), F32),
        dg=vm((1, L), F32),
        stat=vm((nz, 2, nq), F32),
        fac=vm((2, nq), F32),
        gt=vm((npl, DUO, nq), BF16),
        dvp=vm((npl, DUO, L), F32),
        dvs=vm((npl, L, L), F32),
        dvo=vm((npl, L, L), F32),
        dut=vm((nz, L, L), F32),
        rx=vm((nrx, L, L), F32),
        de=vm((DUO, L), F32),
        ga=vm((p.n1[0] * a1, L), F32),
        gb=vm((HALF_ROWS, L), F32),
        r1a=vm((most, a1, L), F32),
        r1b=vm((most, p.c1[1], L), F32),
        s1a=vm((a1, L), F32),
        s1b=vm((p.c1[1], L), F32),
        r2a=vm((most, p.c2 + SUB, L), F32),
        r2b=vm((most, p.c2, L), F32),
        s2=vm((nz * 2 * p.w + p.tail, L), F32),
        r3=vm((nz, 2 * p.w + p.tail, L), F32),
        f2=vm((nz * 2 * p.w, L), F32),
        lossb=vm((2, SUB, L), F32),
        ld=dma((3 + 2 * 4,)),
        sm_s=dma((3,)),
        sm_r=dma((3,)),
        v_s=dma((npl,)),
        v_r=dma((npl,)),
        fw_s=dma((npl,)),
        fw_r=dma((npl,)),
        u_s=dma((nz,)),
        u_r=dma((nz,)),
        ac_s=dma((3,)),
        ac_r=dma((3,)),
        st_s=dma((nz,)),
        st_r=dma((nz,)),
        dv_s=dma((npl,)),
        dv_r=dma((npl,)),
        do_s=dma((npl,)),
        du_s=dma((nz,)),
        rx_r=dma((nrx,)),
        p1_s=dma((2, most)),
        p1_r=dma((2, most)),
        p2_s=dma((3, most)),
        p2_r=dma((3, most)),
        p3_s=dma((2, nz)),
        p3_r=dma((2, nz)),
        p4_s=dma((nz,)),
        p4_r=dma((nz,)),
        p5_s=dma((2, most)),
        p5_r=dma((2, most)),
        p6_s=dma((2, most)),
        p6_r=dma((2, most)),
        sb_s=dma((2, most)),
        sb_r=dma((2, most)),
        ls_s=dma(()),
        ls_r=dma(()),
    )


def _kernel(p, names, ux, ix, ids, lq, uw1, uw2, uw3, iw1, iw2, iw3, fin, loss, *refs):
    s = dict(zip(names, refs, strict=True))
    nz, ny, nx, npl, nq = p.nz, p.ny, p.nx, p.plane, p.queries
    half = nz // 2
    mark = _Marks()
    me = lax.axis_index("dp")
    c = lax.rem(me, 2)
    chip = lax.div(me, 2)
    x = lax.rem(chip, nx)
    y = lax.rem(lax.div(chip, nx), ny)
    z = lax.div(chip, nx * ny)
    sibling = me + 1 - 2 * c

    def dev(dz, dy, dx, core):
        zz, yy, xx = lax.rem(z + dz, nz), lax.rem(y + dy, ny), lax.rem(x + dx, nx)
        return ((zz * ny + yy) * nx + xx) * 2 + core

    def rcopy(src, dst, send, recv, to):
        return pltpu.make_async_remote_copy(
            src_ref=src, dst_ref=dst, send_sem=send, recv_sem=recv, device_id=(to,), device_id_type=MESH
        )

    sends = []

    def send(src, dst, ssem, rsem, to):
        cp = rcopy(src, dst, ssem, rsem, to)
        cp.start()
        sends.append(cp)

    def arrived(dst, rsem):
        rcopy(dst, dst, rsem, rsem, me).wait_recv()

    lane = pl.ds(pl.multiple_of(c * L, L), L)
    other = pl.ds(pl.multiple_of((1 - c) * L, L), L)

    mark("start")
    xs, idb, lqb, idq, ld = s["xs"], s["idb"], s["lqb"], s["idq"], s["ld"]
    own = p.own
    small = [(ids, idb.at[c]), (lq, lqb.at[c]), (ids, idq.at[own])]
    small = [pltpu.make_async_copy(a, b, ld.at[i]) for i, (a, b) in enumerate(small)]
    loads = {}
    n_ld = len(small)
    for t, given in ((ITEM, (ix, iw1, iw2, iw3)), (USER, (ux, uw1, uw2, uw3))):
        loads[t] = []
        for src, dst in zip(given, (xs, s["wf1"], s["wf2"], s["wf3"]), strict=True):
            loads[t].append(pltpu.make_async_copy(src, dst.at[t], ld.at[n_ld]))
            n_ld += 1
    for cp in small + loads[ITEM] + loads[USER]:
        cp.start()

    barrier = pltpu.get_barrier_semaphore()
    others = [dev(0, dy, dx, core) for core in PAIR for dy, dx in p.offsets[1:]]
    others += [dev(dz, 0, 0, core) for core in PAIR for dz in _peers(nz)]
    others.append(sibling)
    for to in others:
        pl.semaphore_signal(barrier, inc=1, device_id=(to,), device_id_type=MESH)

    acts, hid, unit = s["acts"], s["hid"], s["unit"]

    def tower(t):
        place = jnp.where(c == t, 0, 1)
        for cp in loads[t]:
            cp.wait()
        w1, w2, w3 = s["wf1"][t].astype(BF16), s["wf2"][t].astype(BF16), s["wf3"][t].astype(BF16)
        s["w2"][t], s["w3"][t] = w2, w3
        xh = xs[t].astype(BF16)
        h1 = jnp.maximum(_dot(xh, w1), 0.0).astype(BF16)
        h2 = jnp.maximum(_dot(h1, w2), 0.0).astype(BF16)
        raw = _dot(h2, w3)
        inv = lax.rsqrt(jnp.sum(raw * raw, axis=1, keepdims=True) + NORM_EPS)
        e = raw * inv
        acts[place, X_AT:H1_AT, lane] = xh.T
        acts[place, H1_AT:H2_AT, lane] = h1.T
        acts[place, H2_AT:ACT_ROWS, lane] = h2.T
        hid[place, lane, :W_A] = h1
        hid[place, lane, W_A:] = h2
        unit[place, lane, :L] = e
        unit[place, lane, L:] = jnp.broadcast_to(inv, (L, L))
        return e.astype(BF16)

    mark("towers")
    vaug, uall = s["vaug"], s["uall"]
    vaug[0, lane, :L] = tower(ITEM)
    uall[_lanes(own), :] = tower(USER)
    for cp in small:
        cp.wait()
    mark("barrier_wait")
    pl.semaphore_wait(barrier, len(others))

    mark("send_uv")
    sm_s, sm_r = s["sm_s"], s["sm_r"]

    def send_small(k, to):
        rcopy(idb.at[c], idb.at[2 * k + c], sm_s.at[0], sm_r.at[0], to).start()
        rcopy(lqb.at[c], lqb.at[2 * k + c], sm_s.at[1], sm_r.at[1], to).start()

    send_small(0, sibling)
    for dy, dx in p.offsets[1:]:
        for core in PAIR:
            send_small(p.slot(-dy, -dx), dev(0, dy, dx, core))
    n_small = 2 * npl - 1
    for dz in _peers(nz):
        rcopy(idq.at[own], idq.at[p.tile(-dz)], sm_s.at[2], sm_r.at[2], dev(dz, 0, 0, c)).start()

    def vpart(k, rows):
        return vaug.at[k, rows, pl.ds(0, L)]

    def upart(j):
        return uall.at[_lanes(j)]

    send(vpart(0, lane), vpart(0, lane), s["fw_s"].at[0], s["fw_r"].at[0], sibling)
    for i in range(1, max(npl, nz)):
        if i < nz:
            dz = p.zorder[-1 - i]
            send(upart(own), upart(p.tile(-dz)), s["u_s"].at[dz], s["u_r"].at[p.tile(-dz)], dev(dz, 0, 0, c))
        if i < npl:
            dy, dx = p.offsets[i]
            k = p.slot(-dy, -dx)
            send(vpart(0, lane), vpart(k, lane), s["v_s"].at[i], s["v_r"].at[k], dev(0, dy, dx, c))
    for i, part in enumerate(((acts, slice(None), lane), (hid, lane, slice(None)), (unit, lane, slice(None)))):
        ref, rows, cols = part
        send(ref.at[1, rows, cols], ref.at[0, rows, cols], s["ac_s"].at[i], s["ac_r"].at[i], sibling)

    mark("small_wait")
    idk, lqk, idc, ut = s["idk"], s["lqk"], s["idc"], s["ut"]
    idk[...] = jnp.full(idk.shape, -1, I32)
    lqk[...] = jnp.full(lqk.shape, -LOW, F32)
    ut[L:, :] = jnp.where(_iota((L, nq), 0) < 3 * MAX_GROUPS, -1.0, 0.0).astype(BF16)
    for i, (ref, n) in enumerate(((idb, n_small), (lqb, n_small), (idq, nz - 1))):
        if n:
            pltpu.make_async_copy(ref.at[pl.ds(0, n)], ref.at[pl.ds(0, n)], sm_r.at[i]).wait()
    mark("turn")
    for g in range(2 * npl):
        row = idb[g]
        idk[g : g + 1, :] = row
        lqk[g : g + 1, :] = lqb[g] * TEMP
        idc[g // 2, _lanes(g % 2), :] = jnp.broadcast_to(row, (L, L)).T

    def parts(q):
        hi = q.astype(BF16).astype(F32)
        mid = (q - hi).astype(BF16).astype(F32)
        return hi, mid, (q - hi - mid).astype(BF16).astype(F32)

    q_all, id_all = lqk[...], idk[...]
    split = parts(jnp.where(id_all < 0, 0.0, q_all))
    turned = jnp.concatenate([*split, jnp.zeros((MAX_GROUPS, L), F32)], axis=0).T.astype(BF16)
    col = _iota((L, L), 1)
    ones = jnp.where(col < 3 * MAX_GROUPS + 3, 1.0, 0.0)
    for g in range(2 * npl):
        keep = jnp.where(col < 3 * MAX_GROUPS, jnp.where(lax.rem(col, MAX_GROUPS) == g, turned.astype(F32), 0.0), ones)
        vaug[g // 2, _lanes(g % 2), L:] = keep.astype(BF16)

    def most(a):
        return jnp.max(jnp.max(a, axis=0, keepdims=True), axis=1, keepdims=True)

    top1 = most(-q_all)
    at_top = -q_all == top1
    id_hi, id_lo = (id_all // (1 << 16)).astype(F32), (id_all % (1 << 16)).astype(F32)
    top_hi = most(jnp.where(at_top, id_hi, -1.0))
    top_lo = most(jnp.where(jnp.logical_and(at_top, id_hi == top_hi), id_lo, -1.0))
    same_top = jnp.logical_and(id_hi == top_hi, id_lo == top_lo)
    top2 = most(jnp.where(same_top, LOW, -q_all))
    top2 = jnp.where(top2 <= LOW, top1, top2)
    id_top = top_hi.astype(I32) * (1 << 16) + top_lo.astype(I32)
    stat = s["stat"]
    bounds = []
    for j in range(nz):
        rest = top2
        if j == own:
            rest = jnp.maximum(top2, -lqb[c] * TEMP)
        bounds.append(jnp.where(idq[j] == id_top, rest, jnp.broadcast_to(top1, (1, L))))
    bound = jnp.concatenate(bounds, axis=1)
    stat[0, :1, :] = bound
    at = L + 3 * MAX_GROUPS
    ut[at : at + 16, :] = jnp.concatenate([-a for a in parts(bound)] + [jnp.zeros((16 - 3, nq), F32)], axis=0).astype(BF16)

    mark("u_wait")
    for j in reversed(range(nz)):
        if j != own:
            arrived(upart(j), s["u_r"].at[j])
        ut[:L, _lanes(j)] = uall[_lanes(j), :].T

    mark("pass1")
    tb, ls, vt, dg = s["tb"], s["ls"], s["vt"], s["dg"]
    ls[...] = jnp.zeros(ls.shape, F32)
    diag = _iota((DUO, L), 0) == _iota((DUO, L), 1) + c * L

    def pass1(k, mine):
        for j in range(half):
            wide = _dot(vaug[k], ut[:, _lanes(2 * j, 2)])
            for i in PAIR:
                r = 2 * j + i
                t = wide[:, _lanes(i)]
                drop = idc[k] == idq[r]
                if mine and r == own:
                    drop = jnp.logical_and(drop, jnp.logical_not(diag))
                    dg[...] = jnp.sum(jnp.where(diag, t, 0.0), axis=0, keepdims=True)
                e = jnp.where(drop, 0.0, jnp.exp2(t * EXP_SCALE))
                tb[k, :, _lanes(r)] = e
                ls[:, _lanes(r)] += jnp.sum(e.reshape(DUO // SUB, SUB, L), axis=0)

    def forward(k):
        arrived(vpart(k, lane), s["v_r"].at[k])
        rcopy(vpart(k, lane), vpart(k, lane), s["fw_s"].at[k], s["fw_r"].at[k], sibling).start()

    def step1(k, _):
        @pl.when(k + LAG_V < npl)
        def _():
            forward(k + LAG_V)

        arrived(vpart(k, other), s["fw_r"].at[k])
        pass1(k, False)
        return 0

    for k in range(1, min(LAG_V, npl - 1) + 1):
        forward(k)
    arrived(vpart(0, other), s["fw_r"].at[0])
    pass1(0, True)
    mark("pass1_loop")
    lax.fori_loop(1, npl, step1, 0)

    mark("stat_send")
    stat[0, 1:, :] = jnp.sum(ls[...], axis=0, keepdims=True)
    for dz in _peers(nz):
        send(stat.at[0], stat.at[nz - dz], s["st_s"].at[dz], s["st_r"].at[nz - dz], dev(dz, 0, 0, c))

    def flip(k, _):
        vt[k] = vaug[k, :, :L].T
        return 0

    lax.fori_loop(0, npl, flip, 0)
    mark("stat_wait")
    for dz in _peers(nz):
        arrived(stat.at[dz], s["st_r"].at[dz])

    def theirs(row, dz):
        a = stat[dz, row : row + 1, :]
        return a if dz == 0 else jnp.concatenate([a[:, _lanes(p.tile(d - dz))] for d in p.zorder], axis=1)

    sums = [theirs(1, dz) for dz in range(nz)]
    tops = [jnp.where(a > 0.0, theirs(0, dz), LOW) for dz, a in enumerate(sums)]
    top = functools.reduce(jnp.maximum, tops)
    total = sum(a * jnp.exp2((b - top) * EXP_SCALE) for a, b in zip(sums, tops, strict=True))
    mine = _lanes(own)
    loss_part = (top[:, mine] - bound[:, mine] - dg[...]) * INV_TEMP + jnp.log(total[:, mine])
    loss_tile = jnp.where(_iota((SUB, L), 0) == 0, loss_part, 0.0)
    fac = s["fac"]
    inv_batch = 1.0 / p.batch
    fac[:1, :] = jnp.exp2((tops[0] - top) * EXP_SCALE) * (1.0 / total)
    fac[1:, :] = fac[:1, :] * inv_batch

    gt, dut, dvp, dvs, dvo, rx = s["gt"], s["dut"], s["dvp"], s["dvs"], s["dvo"], s["rx"]
    plane = y * nx + x

    def grads(k, tiles, mine):
        for r in tiles:
            if mine and r == own:
                g = (tb[k, :, _lanes(r)] * fac[:1, _lanes(r)] - jnp.where(diag, 1.0, 0.0)) * inv_batch
            else:
                g = tb[k, :, _lanes(r)] * fac[1:, _lanes(r)]
            gt[k, :, _lanes(r)] = g.astype(BF16)
        first = tiles[0]
        for j in range(len(tiles) // 2):
            part = _dot(vt[k], gt[k, :, _lanes(first + 2 * j, 2)])
            for i in PAIR:
                r = first + 2 * j + i
                piece = part[:, _lanes(i)]
                dut[r] = piece if mine else dut[r] + piece

    def send_du(tiles):
        for j in tiles:
            dz = p.zorder[j]
            if dz:
                send(dut.at[j], rx.at[2 * z + c], s["du_s"].at[dz], s["rx_r"].at[2 * z + c], dev(dz, 0, 0, 0))

    def chip_sum(k):
        arrived(dvs.at[k], s["dv_r"].at[k])
        return dvp[k, lane, :] + dvs[k]

    def finish(k):
        dvo[k] = chip_sum(k)
        to = dev(0, _near(lax.div(k, nx)), _near(lax.rem(k, nx)), 1)
        rcopy(dvo.at[k], rx.at[2 * plane + c], s["do_s"].at[k], s["rx_r"].at[2 * plane + c], to).start()

    far, close = range(half), range(half, nz)
    mark("pass2a")
    grads(0, far, True)

    def step2a(k, _):
        grads(k, far, False)
        return 0

    lax.fori_loop(1, npl, step2a, 0)
    send_du(far)

    mark("pass2b")

    def item_part(k):
        dvp[k] = _dot(gt[k], uall[...])
        rcopy(dvp.at[k, other], dvs.at[k], s["dv_s"].at[k], s["dv_r"].at[k], sibling).start()

    grads(0, close, True)

    def step2b(i, _):
        k = npl - 1 - i
        grads(k, close, False)
        item_part(k)

        @pl.when(i >= LAG_DV)
        def _():
            finish(k + LAG_DV)

        return 0

    lax.fori_loop(0, npl - 1, step2b, 0)
    mark("rs_send")
    send_du(close)
    item_part(0)
    for k in reversed(range(1, min(LAG_DV, npl - 1) + 1)):
        finish(k)
    dvo[0] = chip_sum(0)

    mark("rs_wait")
    de = s["de"]

    def gather(h, acc, order, turn):
        for j in order:
            arrived(rx.at[j], s["rx_r"].at[j])
            acc = rx[j] if acc is None else acc + rx[j]
        de[_lanes(h), :] = (acc.T if turn else acc) * INV_TEMP

    z_from = [lax.rem(z + d, nz) for d in p.zorder if d]
    plane_from = [
        lax.rem(y + ny - dy, ny) * nx + lax.rem(x + nx - dx, nx) for dy, dx in reversed(p.offsets[1:])
    ]

    @pl.when(c == USER)
    def _():
        cp = rcopy(dvo.at[0], rx.at[2 * plane], s["do_s"].at[0], s["rx_r"].at[2 * plane], sibling)
        cp.start()
        gather(0, dut[own], [2 * a for a in z_from], True)
        gather(1, None, [2 * a + 1 for a in [*z_from, z]], True)
        cp.wait_send()

    @pl.when(c == ITEM)
    def _():
        cp = rcopy(dut.at[own], rx.at[2 * z + 1], s["du_s"].at[0], s["rx_r"].at[2 * z + 1], sibling)
        cp.start()
        gather(1, dvo[0], [2 * a + 1 for a in plane_from], False)
        gather(0, None, [2 * a for a in [*plane_from, plane]], False)
        cp.wait_send()

    mark("backward")
    arrived(acts.at[0, :, other], s["ac_r"].at[0])
    arrived(hid.at[0, other, :], s["ac_r"].at[1])
    arrived(unit.at[0, other, :], s["ac_r"].at[2])
    ga, gb = s["ga"], s["gb"]
    c1a, c1b = p.c1
    stride1 = (c1a + SUB, c1b)

    def put(start, val):
        n, done = val.shape[0], 0
        while done < n:
            row = start + done
            color = row // HALF_ROWS
            row -= color * HALF_ROWS
            size = p.c1[color]
            chunk, off = row // size, row % size
            take = min(n - done, size - off)
            to = chunk * stride1[color] + off
            (ga, gb)[color][to : to + take, :] = val[done : done + take]
            done += take

    for i in range(nx):
        ga[(i + 1) * stride1[0] - SUB : (i + 1) * stride1[0], :] = loss_tile
    de_all = de[...]
    e, inv = unit[0, :, :L], unit[0, :, L:]
    dz_h = (inv * (de_all - e * jnp.sum(e * de_all, axis=1, keepdims=True))).astype(BF16)
    put(AT_3, _dot(acts[0, H2_AT:ACT_ROWS, :], dz_h))
    da2 = jnp.where(hid[0, :, W_A:] > 0, _dot(dz_h, s["w3"][c], NT), 0.0).astype(BF16)
    dw2 = _dot(acts[0, H1_AT:H2_AT, :], da2)
    for j in range(COLS):
        put(AT_2 + W_A * j, dw2[:, _lanes(j)])
    da1 = jnp.where(hid[0, :, :W_A] > 0, _dot(da2, s["w2"][c], NT), 0.0).astype(BF16)
    dw1 = _dot(acts[0, X_AT:H1_AT, :], da1)
    for j in range(COLS):
        put(W_IN * j, dw1[:, _lanes(j)])

    mark("ar1_send")
    q1, q2 = (x, y), (y, x)
    g, r1, s1, r2 = (ga, gb), (s["r1a"], s["r1b"]), (s["s1a"], s["s1b"]), (s["r2a"], s["r2b"])
    c2, w, rest, tail = p.c2, p.w, p.rest, p.tail

    def along(axis_x, d):
        return dev(0, 0, d, c) if axis_x else dev(0, d, 0, c)

    def along1(color, d):
        return along(color == 0, d)

    def along2(color, d):
        return along(color == 1, d)

    for d in _peers(max(nx, ny)):
        for color in PAIR:
            n1, st = p.n1[color], stride1[color]
            if d < n1:
                at = _at(lax.rem(q1[color] + d, n1) * st, st)
                send(g[color].at[at], r1[color].at[d], s["p1_s"].at[color, d], s["p1_r"].at[color, d], along1(color, d))
    mark("ar1_wait")
    loss_rows = slice(c1a, c1a + SUB)
    loss_in = slice(c2, c2 + SUB)
    for color in PAIR:
        st = stride1[color]
        acc = g[color][_at(q1[color] * st, st), :]
        for d in _peers(p.n1[color]):
            arrived(r1[color].at[d], s["p1_r"].at[color, d])
            acc = acc + r1[color][d]
        s1[color][...] = acc
        for d in _peers(p.n2[color]):
            at, to = _at(lax.rem(q2[color] + d, p.n2[color]) * c2, c2), along2(color, d)
            send(s1[color].at[at], r2[color].at[d, :c2], s["p2_s"].at[color, d], s["p2_r"].at[color, d], to)
            if color == 0:
                send(s1[0].at[loss_rows], r2[0].at[d, loss_in], s["p2_s"].at[2, d], s["p2_r"].at[2, d], to)
    mark("ar2_wait")
    s2, r3, f2, lossb = s["s2"], s["r3"], s["f2"], s["lossb"]
    base = nz * 2 * w
    for color in PAIR:
        acc = s1[color][_at(q2[color] * c2, c2), :]
        for d in _peers(p.n2[color]):
            arrived(r2[color].at[d, :c2], s["p2_r"].at[color, d])
            acc = acc + r2[color][d, :c2, :]
        for i in range(nz):
            at = (2 * i + color) * w
            s2[at : at + w, :] = acc[i * w : (i + 1) * w]
        if rest:
            s2[base + color * rest : base + (color + 1) * rest, :] = acc[nz * w :]
    acc = s1[0][loss_rows, :]
    for d in _peers(p.n2[0]):
        arrived(r2[0].at[d, loss_in], s["p2_r"].at[2, d])
        acc = acc + r2[0][d, loss_in, :]
    s2[base + 2 * rest :, :] = acc
    own_units, shared = slice(0, 2 * w), slice(2 * w, 2 * w + tail)
    for dz in _peers(nz):
        at, to = _at(lax.rem(z + dz, nz) * 2 * w, 2 * w), dev(dz, 0, 0, c)
        send(s2.at[at], r3.at[dz, own_units], s["p3_s"].at[0, dz], s["p3_r"].at[0, dz], to)
        send(s2.at[base:], r3.at[dz, shared], s["p3_s"].at[1, dz], s["p3_r"].at[1, dz], to)
    mark("ar3_wait")
    mine = _at(z * 2 * w, 2 * w)
    acc = s2[mine, :]
    for dz in _peers(nz):
        arrived(r3.at[dz, own_units], s["p3_r"].at[0, dz])
        acc = acc + r3[dz, own_units, :]
    f2[mine, :] = acc
    for dz in _peers(nz):
        send(f2.at[mine], f2.at[mine], s["p4_s"].at[dz], s["p4_r"].at[nz - dz], dev(dz, 0, 0, c))
    acc_shared = s2[base:, :]
    for dz in _peers(nz):
        arrived(r3.at[dz, shared], s["p3_r"].at[1, dz])
        acc_shared = acc_shared + r3[dz, shared, :]
    lossb[c] = acc_shared[2 * rest :]
    send(lossb.at[c], lossb.at[c], s["ls_s"], s["ls_r"], sibling)
    mark("ar4_wait")
    for dz in _peers(nz):
        arrived(f2.at[_at(lax.rem(z + dz, nz) * 2 * w, 2 * w)], s["p4_r"].at[dz])
    for color in PAIR:
        start = color * HALF_ROWS + q1[color] * p.c1[color] + q2[color] * c2
        for i in range(nz):
            at = (2 * i + color) * w
            fin[c, _at(start + i * w, w), :] = f2[at : at + w, :]
        if rest:
            fin[c, _at(start + nz * w, rest), :] = acc_shared[color * rest : (color + 1) * rest]
        place = fin.at[c, _at(start, c2)]
        for d in _peers(p.n2[color]):
            send(place, place, s["p5_s"].at[color, d], s["p5_r"].at[color, p.n2[color] - d], along2(color, d))
    mark("ar5_wait")

    def chunk(color, tower_index, d):
        start = color * HALF_ROWS + lax.rem(q1[color] + d, p.n1[color]) * p.c1[color]
        return fin.at[tower_index, _at(start, p.c1[color])]

    def share(color, d):
        send(chunk(color, c, d), chunk(color, c, d), s["sb_s"].at[color, d], s["sb_r"].at[color, d], sibling)

    for color in PAIR:
        n1, n2 = p.n1[color], p.n2[color]
        for d in _peers(n2):
            start = color * HALF_ROWS + q1[color] * p.c1[color] + lax.rem(q2[color] + d, n2) * c2
            arrived(fin.at[c, _at(start, c2)], s["p5_r"].at[color, d])
        place = chunk(color, c, 0)
        for d in _peers(n1):
            send(place, place, s["p6_s"].at[color, d], s["p6_r"].at[color, n1 - d], along1(color, d))
        share(color, 0)
    mark("ar6_wait")
    for d in _peers(max(p.n1)):
        for color in PAIR:
            if d < p.n1[color]:
                arrived(chunk(color, c, d), s["p6_r"].at[color, d])
                share(color, d)
    mark("sib_wait")
    arrived(lossb.at[1 - c], s["ls_r"])
    loss[...] = jnp.sum(lossb[0] + lossb[1], axis=1, keepdims=True)[:1] * inv_batch + jnp.zeros(loss.shape, F32)
    for d in range(max(p.n1)):
        for color in PAIR:
            if d < p.n1[color]:
                arrived(chunk(color, 1 - c, d), s["sb_r"].at[color, d])

    mark("final_waits")
    for i, (ref, n) in enumerate(((idb, n_small), (lqb, n_small), (idq, nz - 1))):
        if n:
            pltpu.make_async_copy(ref.at[pl.ds(0, n)], ref.at[pl.ds(0, n)], sm_s.at[i]).wait()

    def left(ref, sem):
        rcopy(ref, ref, sem, sem, sibling).wait_send()

    def sent(k, _):
        left(vpart(k, lane), s["fw_s"].at[k])
        left(dvo.at[k], s["do_s"].at[k])
        left(dvs.at[k], s["dv_s"].at[k])
        return 0

    lax.fori_loop(1, npl, sent, 0)
    left(dvs.at[0], s["dv_s"].at[0])
    for cp in sends:
        cp.wait_send()
    mark()


def _layout_kernel(fin, loss_in, *refs):
    outs, sem = refs[:-1], refs[-1]
    copies = []

    def put(src, dst):
        cp = pltpu.make_async_copy(src, dst, sem.at[len(copies)])
        cp.start()
        copies.append(cp)

    for t in PAIR:
        o1, o2, o3 = outs[COLS * t : COLS * (t + 1)]
        for j in range(COLS):
            put(fin.at[t, W_IN * j : W_IN * (j + 1)], o1.at[:, _lanes(j)])
            put(fin.at[t, AT_2 + W_A * j : AT_2 + W_A * (j + 1)], o2.at[:, _lanes(j)])
        put(fin.at[t, AT_3:], o3)
    outs[-1][0, 0] = jnp.max(loss_in[...])
    for cp in copies:
        cp.wait()


def _step(p, ux, ix, ids, lq, uw1, uw2, uw3, iw1, iw2, iw3):
    scratch = _scratch(p)
    anywhere, vmem = pl.BlockSpec(memory_space=pl.ANY), pl.BlockSpec(memory_space=pltpu.VMEM)
    fin, loss = pl.pallas_call(
        functools.partial(_kernel, p, tuple(scratch)),
        out_shape=(pltpu.VMEM((2, GRAD_ROWS, L), F32), pltpu.VMEM((SUB, L), F32)),
        in_specs=[anywhere] * len((ux, ix, ids, lq, uw1, uw2, uw3, iw1, iw2, iw3)),
        out_specs=(vmem, vmem),
        scratch_shapes=list(scratch.values()),
        compiler_params=pltpu.CompilerParams(collective_id=0, has_side_effects=True, vmem_limit_bytes=VMEM_BYTES),
        name="two_tower_step",
    )(ux, ix, ids.reshape(1, L), lq.reshape(1, L), uw1, uw2, uw3, iw1, iw2, iw3)
    shapes = [(W_IN, W_A), (W_A, W_B), (W_B, L)] * 2
    *grads, loss = pl.pallas_call(
        _layout_kernel,
        out_shape=[jax.ShapeDtypeStruct(a, F32) for a in [*shapes, (1, 1)]],
        in_specs=[vmem, vmem],
        out_specs=[anywhere] * len(shapes) + [pl.BlockSpec(memory_space=pltpu.SMEM)],
        scratch_shapes=[pltpu.SemaphoreType.DMA((2 * (2 * COLS + 1),))],
        compiler_params=pltpu.CompilerParams(vmem_limit_bytes=LAYOUT_BYTES),
        name="layout",
    )(fin, loss)
    return (loss.reshape(()), *grads)


def solution(mesh):
    p = _Plan(mesh.shape["dp"])
    rows, vec, whole = P("dp", None), P("dp"), P()
    return jax.shard_map(
        functools.partial(_step, p),
        mesh=mesh,
        in_specs=(rows, rows, vec, vec, whole, whole, whole, whole, whole, whole),
        out_specs=(whole,) * (1 + 2 * COLS),
        check_vma=False,
    )
```

```python
import functools
import math

import jax
import jax.numpy as jnp
from jax import lax
from jax.experimental import pallas as pl
from jax.experimental.pallas import tpu as pltpu
from jax.sharding import PartitionSpec as P

F32, BF16, I32 = jnp.float32, jnp.bfloat16, jnp.int32
MESH = pl.DeviceIdType.MESH

GRID = {256: (8, 4, 4)}

L, SUB = 128, 8
PAIR = range(2)
USER, ITEM = PAIR
W_IN, W_A, W_B = 256, 384, 384
DUO = 2 * L
MAX_GROUPS = 32
TEMP = 0.05
INV_TEMP = 1.0 / TEMP
EXP_SCALE = INV_TEMP * math.log2(math.e)
NORM_EPS = 1e-6
LOW = -3.0e38
ROWS_1, ROWS_2, ROWS_3 = W_IN * W_A // L, W_A * W_B // L, W_B
AT_3, AT_2, AT_1 = 0, ROWS_3, ROWS_3 + ROWS_2
GRAD_ROWS = AT_1 + ROWS_1
STREAM, STREAM_C = 512, 256
AT_C = 2 * STREAM
STREAMS = (0, STREAM, AT_C + STREAM_C, AT_C + STREAM_C + STREAM)
COLS = W_A // L
X_AT, H1_AT, H2_AT, ACT_ROWS = 0, W_IN, W_IN + W_A, W_IN + W_A + W_B
GROUP = 4
VMEM_BYTES, LAYOUT_BYTES = 56 << 20, 1 << 20
NN = (((1,), (0,)), ((), ()))
NT = (((1,), (1,)), ((), ()))


def _dot(a, b, dims=NN):
    return lax.dot_general(a, b, dims, preferred_element_type=F32)


def _near(k):
    return k + k // 2 - 2 * (k // 3)


def _lanes(j, n=1):
    return slice(j * L, (j + n) * L)


def _at(start, size):
    return pl.ds(pl.multiple_of(start, SUB), size)


def _peers(n):
    return range(1, n)


def _iota(shape, dim):
    return lax.broadcasted_iota(I32, shape, dim)


class _Marks:
    def __init__(self):
        self.scope = None

    def __call__(self, name=None):
        if self.scope is not None:
            self.scope.__exit__(None, None, None)
        self.scope = jax.named_scope(name) if name else None
        if name:
            self.scope.__enter__()


class _Plan:
    def __init__(self, n):
        nz, ny, nx = self.nz, self.ny, self.nx = GRID[n]
        self.plane = nx * ny
        self.batch = n * L
        self.queries = nz * L
        self.ch1 = tuple(STREAM // m for m in (nx, ny))
        self.ch2 = STREAM // self.plane
        self.zc = 2 * self.ch2 // nz
        self.cz = STREAM_C // nz
        self.cx = self.cz // nx
        self.offsets = [(_near(k // nx), _near(k % nx)) for k in range(self.plane)]
        self.zorder = sorted(range(nz), key=lambda d: -min(d, nz - d))
        self.own = self.zorder.index(0)

    def slot(self, dy, dx):
        return self.offsets.index((dy % self.ny, dx % self.nx))

    def tile(self, dz):
        return self.zorder.index(dz % self.nz)


def _scratch(p):
    npl, nz, nq = p.plane, p.nz, p.queries
    vm, dma = pltpu.VMEM, pltpu.SemaphoreType.DMA
    groups, most = 2 * npl, max(p.nx, p.ny)
    nrx = max(groups, 2 * nz)
    chunk = max(p.ch1)
    items = npl * DUO
    return dict(
        xs=vm((2, L, W_IN), F32),
        wf1=vm((2, W_IN, W_A), F32),
        wf2=vm((2, W_A, W_B), F32),
        wf3=vm((2, W_B, L), F32),
        w2=vm((2, W_A, W_B), BF16),
        w3=vm((2, W_B, L), BF16),
        acts=vm((2, ACT_ROWS, DUO), BF16),
        hid=vm((2, DUO, W_A + W_B), BF16),
        unit=vm((2, DUO, DUO), F32),
        idb=vm((groups, 1, L), I32),
        lqb=vm((groups, 1, L), F32),
        idq=vm((nz, 1, L), I32),
        idk=vm((MAX_GROUPS, L), I32),
        lqk=vm((MAX_GROUPS, L), F32),
        idc=vm((items, L), I32),
        vaug=vm((items, DUO), BF16),
        vt=vm((L, items), BF16),
        uall=vm((nq, L), BF16),
        ut=vm((DUO, nq), BF16),
        tb=vm((items, nq), F32),
        ls=vm((SUB, nq), F32),
        dg=vm((1, L), F32),
        stat=vm((nz, 2, nq), F32),
        fac=vm((2, nq), F32),
        gt=vm((items, nq), BF16),
        dvp=vm((items, L), F32),
        dvs=vm((npl, L, L), F32),
        dvo=vm((npl, L, L), F32),
        dut=vm((nz, L, L), F32),
        rx=vm((nrx, L, L), F32),
        de=vm((DUO, L), F32),
        g=vm((GRAD_ROWS, L), F32),
        gc=vm((nz * (p.cz + SUB), L), F32),
        r1=vm((4, most, chunk, L), F32),
        s1=vm((4, chunk, L), F32),
        r2=vm((4, most, p.ch2, L), F32),
        s2=vm((2, 2 * p.ch2, L), F32),
        r3=vm((2, nz, p.zc, L), F32),
        rc1=vm((nz, p.cz + SUB, L), F32),
        sc1=vm((p.cz + SUB, L), F32),
        rc2=vm((p.nx, p.cx + SUB, L), F32),
        rc3=vm((p.ny, p.cx + SUB, L), F32),
        lossb=vm((2, SUB, L), F32),
        ld=dma((3 + 2 * 4,)),
        sm_s=dma((3,)),
        sm_r=dma((3,)),
        v_s=dma((npl,)),
        v_r=dma((npl,)),
        fw_s=dma((npl,)),
        fw_r=dma((npl,)),
        u_s=dma((nz,)),
        u_r=dma((nz,)),
        ac_s=dma((3,)),
        ac_r=dma((3,)),
        st_s=dma((nz,)),
        st_r=dma((nz,)),
        dv_s=dma((npl,)),
        dv_r=dma((npl,)),
        do_s=dma((npl,)),
        du_s=dma((nz,)),
        rx_r=dma((nrx,)),
        p1_s=dma((4, most)),
        p1_r=dma((4, most)),
        p2_s=dma((4, most)),
        p2_r=dma((4, most)),
        p3_s=dma((2, nz)),
        p3_r=dma((2, nz)),
        p4_s=dma((2, nz)),
        p4_r=dma((2, nz)),
        p5_s=dma((4, most)),
        p5_r=dma((4, most)),
        p6_s=dma((4, most)),
        p6_r=dma((4, most)),
        sb_s=dma((4 + 1, most)),
        sb_r=dma((4 + 1, most)),
        c1_s=dma((nz,)),
        c1_r=dma((nz,)),
        c2_s=dma((2, p.nx)),
        c2_r=dma((2, p.nx)),
        c3_s=dma((p.ny,)),
        c3_r=dma((p.ny,)),
        c4_s=dma((p.nx,)),
        c4_r=dma((p.nx,)),
        c5_s=dma((nz,)),
        c5_r=dma((nz,)),
        ls_s=dma(()),
        ls_r=dma(()),
    )


def _kernel(p, names, ux, ix, ids, lq, uw1, uw2, uw3, iw1, iw2, iw3, fin, loss, *refs):
    s = dict(zip(names, refs, strict=True))
    nz, ny, nx, npl, nq = p.nz, p.ny, p.nx, p.plane, p.queries
    half = nz // 2
    mark = _Marks()
    me = lax.axis_index("dp")
    c = lax.rem(me, 2)
    chip = lax.div(me, 2)
    x = lax.rem(chip, nx)
    y = lax.rem(lax.div(chip, nx), ny)
    z = lax.div(chip, nx * ny)
    sibling = me + 1 - 2 * c

    def dev(dz, dy, dx, core):
        zz, yy, xx = lax.rem(z + dz, nz), lax.rem(y + dy, ny), lax.rem(x + dx, nx)
        return ((zz * ny + yy) * nx + xx) * 2 + core

    def rcopy(src, dst, send, recv, to):
        return pltpu.make_async_remote_copy(
            src_ref=src, dst_ref=dst, send_sem=send, recv_sem=recv, device_id=(to,), device_id_type=MESH
        )

    sends = []

    def send(src, dst, ssem, rsem, to):
        cp = rcopy(src, dst, ssem, rsem, to)
        cp.start()
        sends.append(cp)

    def arrived(dst, rsem):
        rcopy(dst, dst, rsem, rsem, me).wait_recv()

    lane = pl.ds(pl.multiple_of(c * L, L), L)
    other = pl.ds(pl.multiple_of((1 - c) * L, L), L)

    mark("start")
    xs, idb, lqb, idq, ld = s["xs"], s["idb"], s["lqb"], s["idq"], s["ld"]
    own = p.own
    small = [(ids, idb.at[c]), (lq, lqb.at[c]), (ids, idq.at[own])]
    small = [pltpu.make_async_copy(a, b, ld.at[i]) for i, (a, b) in enumerate(small)]
    loads = {}
    n_ld = len(small)
    for t, given in ((ITEM, (ix, iw1, iw2, iw3)), (USER, (ux, uw1, uw2, uw3))):
        loads[t] = []
        for src, dst in zip(given, (xs, s["wf1"], s["wf2"], s["wf3"]), strict=True):
            loads[t].append(pltpu.make_async_copy(src, dst.at[t], ld.at[n_ld]))
            n_ld += 1
    for cp in small + loads[ITEM] + loads[USER]:
        cp.start()

    barrier = pltpu.get_barrier_semaphore()
    others = [dev(0, dy, dx, core) for core in PAIR for dy, dx in p.offsets[1:]]
    others += [dev(dz, 0, 0, core) for core in PAIR for dz in _peers(nz)]
    others.append(sibling)
    for to in others:
        pl.semaphore_signal(barrier, inc=1, device_id=(to,), device_id_type=MESH)

    acts, hid, unit = s["acts"], s["hid"], s["unit"]

    def tower(t):
        place = jnp.where(c == t, 0, 1)
        for cp in loads[t]:
            cp.wait()
        w1, w2, w3 = s["wf1"][t].astype(BF16), s["wf2"][t].astype(BF16), s["wf3"][t].astype(BF16)
        s["w2"][t], s["w3"][t] = w2, w3
        xh = xs[t].astype(BF16)
        h1 = jnp.maximum(_dot(xh, w1), 0.0).astype(BF16)
        h2 = jnp.maximum(_dot(h1, w2), 0.0).astype(BF16)
        raw = _dot(h2, w3)
        inv = lax.rsqrt(jnp.sum(raw * raw, axis=1, keepdims=True) + NORM_EPS)
        e = raw * inv
        acts[place, X_AT:H1_AT, lane] = xh.T
        acts[place, H1_AT:H2_AT, lane] = h1.T
        acts[place, H2_AT:ACT_ROWS, lane] = h2.T
        hid[place, lane, :W_A] = h1
        hid[place, lane, W_A:] = h2
        unit[place, lane, :L] = e
        unit[place, lane, L:] = jnp.broadcast_to(inv, (L, L))
        return e.astype(BF16)

    mark("towers")
    vaug, uall = s["vaug"], s["uall"]
    vaug[lane, :L] = tower(ITEM)
    uall[_lanes(own), :] = tower(USER)
    for cp in small:
        cp.wait()
    mark("barrier_wait")
    pl.semaphore_wait(barrier, len(others))

    mark("send_uv")
    sm_s, sm_r = s["sm_s"], s["sm_r"]

    def send_small(k, to):
        rcopy(idb.at[c], idb.at[2 * k + c], sm_s.at[0], sm_r.at[0], to).start()
        rcopy(lqb.at[c], lqb.at[2 * k + c], sm_s.at[1], sm_r.at[1], to).start()

    send_small(0, sibling)
    for dy, dx in p.offsets[1:]:
        for core in PAIR:
            send_small(p.slot(-dy, -dx), dev(0, dy, dx, core))
    n_small = 2 * npl - 1
    for dz in _peers(nz):
        rcopy(idq.at[own], idq.at[p.tile(-dz)], sm_s.at[2], sm_r.at[2], dev(dz, 0, 0, c)).start()

    def vpart(k, core):
        return vaug.at[pl.ds(pl.multiple_of(k * DUO + core * L, L), L), pl.ds(0, L)]

    def upart(j):
        return uall.at[_lanes(j)]

    send(vpart(0, c), vpart(0, c), s["fw_s"].at[0], s["fw_r"].at[0], sibling)
    for i in range(1, max(npl, nz)):
        if i < nz:
            dz = p.zorder[-1 - i]
            send(upart(own), upart(p.tile(-dz)), s["u_s"].at[dz], s["u_r"].at[p.tile(-dz)], dev(dz, 0, 0, c))
        if i < npl:
            dy, dx = p.offsets[i]
            k = p.slot(-dy, -dx)
            send(vpart(0, c), vpart(k, c), s["v_s"].at[i], s["v_r"].at[k], dev(0, dy, dx, c))
    for i, part in enumerate(((acts, slice(None), lane), (hid, lane, slice(None)), (unit, lane, slice(None)))):
        ref, rows, cols = part
        send(ref.at[1, rows, cols], ref.at[0, rows, cols], s["ac_s"].at[i], s["ac_r"].at[i], sibling)

    mark("small_wait")
    idk, lqk, idc, ut = s["idk"], s["lqk"], s["idc"], s["ut"]
    idk[...] = jnp.full(idk.shape, -1, I32)
    lqk[...] = jnp.full(lqk.shape, -LOW, F32)
    ut[L:, :] = jnp.where(_iota((L, nq), 0) < 3 * MAX_GROUPS, -1.0, 0.0).astype(BF16)
    for i, (ref, n) in enumerate(((idb, n_small), (lqb, n_small), (idq, nz - 1))):
        if n:
            pltpu.make_async_copy(ref.at[pl.ds(0, n)], ref.at[pl.ds(0, n)], sm_r.at[i]).wait()
    mark("turn")
    for g in range(2 * npl):
        row = idb[g]
        idk[g : g + 1, :] = row
        lqk[g : g + 1, :] = lqb[g] * TEMP
        idc[_lanes(g), :] = jnp.broadcast_to(row, (L, L)).T

    def parts(q):
        hi = q.astype(BF16).astype(F32)
        mid = (q - hi).astype(BF16).astype(F32)
        return hi, mid, (q - hi - mid).astype(BF16).astype(F32)

    q_all, id_all = lqk[...], idk[...]
    split = parts(jnp.where(id_all < 0, 0.0, q_all))
    turned = jnp.concatenate([*split, jnp.zeros((MAX_GROUPS, L), F32)], axis=0).T.astype(BF16)
    col = _iota((L, L), 1)
    ones = jnp.where(col < 3 * MAX_GROUPS + 3, 1.0, 0.0)
    for g in range(2 * npl):
        keep = jnp.where(col < 3 * MAX_GROUPS, jnp.where(lax.rem(col, MAX_GROUPS) == g, turned.astype(F32), 0.0), ones)
        vaug[_lanes(g), L:] = keep.astype(BF16)

    def most(a):
        return jnp.max(jnp.max(a, axis=0, keepdims=True), axis=1, keepdims=True)

    top1 = most(-q_all)
    at_top = -q_all == top1
    id_hi, id_lo = (id_all // (1 << 16)).astype(F32), (id_all % (1 << 16)).astype(F32)
    top_hi = most(jnp.where(at_top, id_hi, -1.0))
    top_lo = most(jnp.where(jnp.logical_and(at_top, id_hi == top_hi), id_lo, -1.0))
    same_top = jnp.logical_and(id_hi == top_hi, id_lo == top_lo)
    top2 = most(jnp.where(same_top, LOW, -q_all))
    top2 = jnp.where(top2 <= LOW, top1, top2)
    id_top = top_hi.astype(I32) * (1 << 16) + top_lo.astype(I32)
    stat = s["stat"]
    bounds = []
    for j in range(nz):
        rest = top2
        if j == own:
            rest = jnp.maximum(top2, -lqb[c] * TEMP)
        bounds.append(jnp.where(idq[j] == id_top, rest, jnp.broadcast_to(top1, (1, L))))
    bound = jnp.concatenate(bounds, axis=1)
    stat[0, :1, :] = bound
    at = L + 3 * MAX_GROUPS
    ut[at : at + 16, :] = jnp.concatenate([-a for a in parts(bound)] + [jnp.zeros((16 - 3, nq), F32)], axis=0).astype(BF16)

    tb, ls, vt, dg = s["tb"], s["ls"], s["vt"], s["dg"]
    ls[...] = jnp.zeros(ls.shape, F32)
    diag = _iota((DUO, L), 0) == _iota((DUO, L), 1) + c * L
    far, close = range(half), range(half, nz)

    def queries(tiles):
        for j in reversed(tiles):
            if j != own:
                arrived(upart(j), s["u_r"].at[j])
            ut[:L, _lanes(j)] = uall[_lanes(j), :].T

    def pass1(blocks, tiles):
        rows = slice(blocks[0] * DUO, (blocks[-1] + 1) * DUO)
        wide = _dot(vaug[rows, :], ut[:, _lanes(tiles[0], len(tiles))])
        for i, r in enumerate(tiles):
            add = 0.0
            for n, k in enumerate(blocks):
                at = slice(k * DUO, (k + 1) * DUO)
                t = wide[n * DUO : (n + 1) * DUO, _lanes(i)]
                drop = idc[at, :] == idq[r]
                if k == 0 and r == own:
                    drop = jnp.logical_and(drop, jnp.logical_not(diag))
                    dg[...] = jnp.sum(jnp.where(diag, t, 0.0), axis=0, keepdims=True)
                e = jnp.where(drop, 0.0, jnp.exp2(t * EXP_SCALE))
                tb[at, _lanes(r)] = e
                add = add + jnp.sum(e.reshape(DUO // SUB, SUB, L), axis=0)
            ls[:, _lanes(r)] += add

    def forward(blocks):
        for k in blocks:
            if k:
                arrived(vpart(k, c), s["v_r"].at[k])
                send(vpart(k, c), vpart(k, c), s["fw_s"].at[k], s["fw_r"].at[k], sibling)

    def whole(blocks):
        for k in blocks:
            arrived(vpart(k, 1 - c), s["fw_r"].at[k])

    size = min(GROUP, npl)
    groups = [range(a, a + size) for a in range(0, npl, size)]
    early = groups[: len(groups) // 2]
    late = groups[len(early) :]
    mark("u_close")
    queries(close)
    mark("pass1_close")
    forward(groups[0])
    for n, blocks in enumerate(early):
        forward(groups[n + 1])
        whole(blocks)
        pass1(blocks, close)
    mark("u_far")
    queries(far)
    mark("pass1_far")
    for blocks in early:
        pass1(blocks, far)
    mark("pass1_late")
    for n, blocks in enumerate(late):
        if n + 1 < len(late):
            forward(late[n + 1])
        whole(blocks)
        pass1(blocks, close)
        pass1(blocks, far)

    mark("stat_send")
    stat[0, 1:, :] = jnp.sum(ls[...], axis=0, keepdims=True)
    for dz in _peers(nz):
        send(stat.at[0], stat.at[nz - dz], s["st_s"].at[dz], s["st_r"].at[nz - dz], dev(dz, 0, 0, c))

    for k in range(2 * npl):
        vt[:, _lanes(k)] = vaug[_lanes(k), :L].T
    mark("stat_wait")
    for dz in _peers(nz):
        arrived(stat.at[dz], s["st_r"].at[dz])

    def theirs(row, dz):
        a = stat[dz, row : row + 1, :]
        return a if dz == 0 else jnp.concatenate([a[:, _lanes(p.tile(d - dz))] for d in p.zorder], axis=1)

    sums = [theirs(1, dz) for dz in range(nz)]
    tops = [jnp.where(a > 0.0, theirs(0, dz), LOW) for dz, a in enumerate(sums)]
    top = functools.reduce(jnp.maximum, tops)
    total = sum(a * jnp.exp2((b - top) * EXP_SCALE) for a, b in zip(sums, tops, strict=True))
    mine = _lanes(own)
    loss_part = (top[:, mine] - bound[:, mine] - dg[...]) * INV_TEMP + jnp.log(total[:, mine])
    loss_tile = jnp.where(_iota((SUB, L), 0) == 0, loss_part, 0.0)
    fac = s["fac"]
    inv_batch = 1.0 / p.batch
    fac[:1, :] = jnp.exp2((tops[0] - top) * EXP_SCALE) * (1.0 / total)
    fac[1:, :] = fac[:1, :] * inv_batch

    gt, dut, dvp, dvs, dvo, rx = s["gt"], s["dut"], s["dvp"], s["dvs"], s["dvo"], s["rx"]
    plane = y * nx + x

    def grads(blocks, tiles):
        for k in blocks:
            at = slice(k * DUO, (k + 1) * DUO)
            for r in tiles:
                if k == 0 and r == own:
                    g = (tb[at, _lanes(r)] * fac[:1, _lanes(r)] - jnp.where(diag, 1.0, 0.0)) * inv_batch
                else:
                    g = tb[at, _lanes(r)] * fac[1:, _lanes(r)]
                gt[at, _lanes(r)] = g.astype(BF16)

    def user_part(blocks, tiles, first):
        rows = slice(blocks[0] * DUO, (blocks[-1] + 1) * DUO)
        part = _dot(vt[:, rows], gt[rows, _lanes(tiles[0], len(tiles))])
        for i, r in enumerate(tiles):
            piece = part[:, _lanes(i)]
            dut[r] = piece if first else dut[r] + piece

    def item_part(blocks):
        rows = slice(min(blocks) * DUO, (max(blocks) + 1) * DUO)
        dvp[rows, :] = _dot(gt[rows, :], uall[...])
        for k in blocks:
            src = dvp.at[pl.ds(pl.multiple_of(k * DUO + (1 - c) * L, L), L)]
            send(src, dvs.at[k], s["dv_s"].at[k], s["dv_r"].at[k], sibling)

    def send_du(tiles):
        for j in tiles:
            dz = p.zorder[j]
            if dz:
                send(dut.at[j], rx.at[2 * z + c], s["du_s"].at[dz], s["rx_r"].at[2 * z + c], dev(dz, 0, 0, 0))

    def finish(blocks):
        for k in blocks:
            arrived(dvs.at[k], s["dv_r"].at[k])
            dvo[k] = dvp[pl.ds(pl.multiple_of(k * DUO + c * L, L), L), :] + dvs[k]
            if k:
                dy, dx = p.offsets[k]
                send(dvo.at[k], rx.at[2 * plane + c], s["do_s"].at[k], s["rx_r"].at[2 * plane + c], dev(0, dy, dx, 1))

    mark("pass2a")
    for n, blocks in enumerate(groups):
        grads(blocks, far)
        user_part(blocks, far, n == 0)
    send_du(far)
    mark("pass2b")
    order, lo = [], npl
    while lo:
        take = min(GROUP if len(order) > 1 else GROUP // 2, lo)
        order.append(range(lo - take, lo))
        lo -= take
    for n, blocks in enumerate(order):
        grads(blocks, close)
        item_part(blocks[::-1])
        user_part(blocks, close, n == 0)
        if n:
            finish(order[n - 1][::-1])
    mark("rs_send")
    send_du(close)
    finish(order[-1][::-1])

    mark("rs_wait")
    de = s["de"]

    def gather(h, acc, order, turn):
        for j in order:
            arrived(rx.at[j], s["rx_r"].at[j])
            acc = rx[j] if acc is None else acc + rx[j]
        de[_lanes(h), :] = (acc.T if turn else acc) * INV_TEMP

    z_from = [lax.rem(z + d, nz) for d in p.zorder if d]
    plane_from = [
        lax.rem(y + ny - dy, ny) * nx + lax.rem(x + nx - dx, nx) for dy, dx in reversed(p.offsets[1:])
    ]

    @pl.when(c == USER)
    def _():
        cp = rcopy(dvo.at[0], rx.at[2 * plane], s["do_s"].at[0], s["rx_r"].at[2 * plane], sibling)
        cp.start()
        gather(0, dut[own], [2 * a for a in z_from], True)
        gather(1, None, [2 * a + 1 for a in [*z_from, z]], True)
        cp.wait_send()

    @pl.when(c == ITEM)
    def _():
        cp = rcopy(dut.at[own], rx.at[2 * z + 1], s["du_s"].at[0], s["rx_r"].at[2 * z + 1], sibling)
        cp.start()
        gather(1, dvo[0], [2 * a + 1 for a in plane_from], False)
        gather(0, None, [2 * a for a in [*plane_from, plane]], False)
        cp.wait_send()

    mark("backward")
    arrived(acts.at[0, :, other], s["ac_r"].at[0])
    arrived(hid.at[0, other, :], s["ac_r"].at[1])
    arrived(unit.at[0, other, :], s["ac_r"].at[2])
    g, gc = s["g"], s["gc"]
    cz, cx, ch2, zc = p.cz, p.cx, p.ch2, p.zc
    stride_c = cz + SUB

    def put(start, val):
        n, done = val.shape[0], 0
        while done < n:
            row = start + done
            if AT_C <= row < AT_C + STREAM_C:
                chunk, off = (row - AT_C) // cz, (row - AT_C) % cz
                take = min(n - done, cz - off)
                to = chunk * stride_c + off
                gc[to : to + take, :] = val[done : done + take]
            else:
                take = n - done if row >= AT_C else min(n - done, AT_C - row)
                g[row : row + take, :] = val[done : done + take]
            done += take

    def toward(along_x, d):
        return dev(0, 0, d, c) if along_x else dev(0, d, 0, c)

    class Stream:
        def __init__(self, i):
            self.i, self.start = i, STREAMS[i]
            self.along_x = i % 2 == 0
            self.n1, self.n2 = (nx, ny) if self.along_x else (ny, nx)
            self.q1, self.q2 = (x, y) if self.along_x else (y, x)
            self.ch1 = STREAM // self.n1

        def to1(self, d):
            return toward(self.along_x, d)

        def to2(self, d):
            return toward(not self.along_x, d)

        def chunk1(self, d):
            return _at(self.start + lax.rem(self.q1 + d, self.n1) * self.ch1, self.ch1)

        def row2(self, d):
            return self.start + self.q1 * self.ch1 + lax.rem(self.q2 + d, self.n2) * ch2

        def sem(self, name, d):
            return s[name].at[self.i, d]

    streams = [Stream(i) for i in range(len(STREAMS))]
    sets = (streams[:2], streams[2:])
    r1, s1, r2, s2, r3, lossb = s["r1"], s["s1"], s["r2"], s["s2"], s["r3"], s["lossb"]
    rc1, sc1, rc2, rc3 = s["rc1"], s["sc1"], s["rc2"], s["rc3"]

    def phase1(pair):
        for d in _peers(max(nx, ny)):
            for st in pair:
                if d < st.n1:
                    send(g.at[st.chunk1(d)], r1.at[st.i, d, : st.ch1], st.sem("p1_s", d), st.sem("p1_r", d), st.to1(d))

    def phase2(pair):
        for st in pair:
            acc = g[st.chunk1(0), :]
            for d in _peers(st.n1):
                arrived(r1.at[st.i, d, : st.ch1], st.sem("p1_r", d))
                acc = acc + r1[st.i, d, : st.ch1, :]
            s1[st.i, : st.ch1, :] = acc
            for d in _peers(st.n2):
                at = _at(lax.rem(st.q2 + d, st.n2) * ch2, ch2)
                send(s1.at[st.i, at], r2.at[st.i, d], st.sem("p2_s", d), st.sem("p2_r", d), st.to2(d))

    def phase3(n, pair):
        for j, st in enumerate(pair):
            acc = s1[st.i, _at(st.q2 * ch2, ch2), :]
            for d in _peers(st.n2):
                arrived(r2.at[st.i, d], st.sem("p2_r", d))
                acc = acc + r2[st.i, d]
            s2[n, j * ch2 : (j + 1) * ch2, :] = acc
        for dz in _peers(nz):
            at = _at(lax.rem(z + dz, nz) * zc, zc)
            send(s2.at[n, at], r3.at[n, dz], s["p3_s"].at[n, dz], s["p3_r"].at[n, dz], dev(dz, 0, 0, c))

    def place(pair, dz):
        zz = lax.rem(z + dz, nz)
        second = lax.div(zz, nz // 2)
        first = pair[0].row2(0) * (1 - second) + pair[1].row2(0) * second
        return fin.at[c, _at(first + lax.rem(zz, nz // 2) * zc, zc)]

    def phase4(n, pair):
        acc = s2[n, _at(z * zc, zc), :]
        for dz in _peers(nz):
            arrived(r3.at[n, dz], s["p3_r"].at[n, dz])
            acc = acc + r3[n, dz]
        place(pair, 0)[...] = acc
        for dz in _peers(nz):
            send(place(pair, 0), place(pair, 0), s["p4_s"].at[n, dz], s["p4_r"].at[n, nz - dz], dev(dz, 0, 0, c))

    def phase5(n, pair):
        for dz in _peers(nz):
            arrived(place(pair, dz), s["p4_r"].at[n, dz])
        for st in pair:
            rows = fin.at[c, _at(st.row2(0), ch2)]
            for d in _peers(st.n2):
                send(rows, rows, st.sem("p5_s", d), st.sem("p5_r", st.n2 - d), st.to2(d))

    def share(rows, i, d):
        send(rows, rows, s["sb_s"].at[i, d], s["sb_r"].at[i, d], sibling)

    def phase6(pair):
        for st in pair:
            for d in _peers(st.n2):
                arrived(fin.at[c, _at(st.row2(d), ch2)], st.sem("p5_r", d))
            rows = fin.at[c, st.chunk1(0)]
            for d in _peers(st.n1):
                send(rows, rows, st.sem("p6_s", d), st.sem("p6_r", st.n1 - d), st.to1(d))
            share(rows, st.i, 0)

    def phase7(pair):
        for d in _peers(max(nx, ny)):
            for st in pair:
                if d < st.n1:
                    rows = fin.at[c, st.chunk1(d)]
                    arrived(rows, st.sem("p6_r", d))
                    share(rows, st.i, d)

    def step_c1():
        for dz in _peers(nz):
            at = _at(lax.rem(z + dz, nz) * stride_c, stride_c)
            send(gc.at[at], rc1.at[dz], s["c1_s"].at[dz], s["c1_r"].at[dz], dev(dz, 0, 0, c))

    def step_c2():
        acc = gc[_at(z * stride_c, stride_c), :]
        for dz in _peers(nz):
            arrived(rc1.at[dz], s["c1_r"].at[dz])
            acc = acc + rc1[dz]
        sc1[...] = acc
        for d in _peers(nx):
            at, to = _at(lax.rem(x + d, nx) * cx, cx), dev(0, 0, d, c)
            send(sc1.at[at], rc2.at[d, :cx], s["c2_s"].at[0, d], s["c2_r"].at[0, d], to)
            send(sc1.at[cz:], rc2.at[d, cx:], s["c2_s"].at[1, d], s["c2_r"].at[1, d], to)

    def step_c3():
        acc, loss_acc = sc1[_at(x * cx, cx), :], sc1[cz:, :]
        for d in _peers(nx):
            arrived(rc2.at[d, :cx], s["c2_r"].at[0, d])
            arrived(rc2.at[d, cx:], s["c2_r"].at[1, d])
            acc, loss_acc = acc + rc2[d, :cx, :], loss_acc + rc2[d, cx:, :]
        rc3[y, :cx, :] = acc
        rc3[y, cx:, :] = loss_acc
        for d in _peers(ny):
            send(rc3.at[y], rc3.at[y], s["c3_s"].at[d], s["c3_r"].at[ny - d], dev(0, d, 0, c))

    def rows_c(dz, d, size):
        return fin.at[c, _at(AT_C + lax.rem(z + dz, nz) * cz + lax.rem(x + d, nx) * (cx if size == cx else 0), size)]

    def step_c4():
        for d in _peers(ny):
            arrived(rc3.at[lax.rem(y + d, ny)], s["c3_r"].at[d])
        acc = rc3[0]
        for d in _peers(ny):
            acc = acc + rc3[d]
        rows = rows_c(0, 0, cx)
        rows[...] = acc[:cx]
        lossb[c] = acc[cx:]
        send(lossb.at[c], lossb.at[c], s["ls_s"], s["ls_r"], sibling)
        for d in _peers(nx):
            send(rows, rows, s["c4_s"].at[d], s["c4_r"].at[nx - d], dev(0, 0, d, c))

    def step_c5():
        for d in _peers(nx):
            arrived(rows_c(0, d, cx), s["c4_r"].at[d])
        rows = rows_c(0, 0, cz)
        for dz in _peers(nz):
            send(rows, rows, s["c5_s"].at[dz], s["c5_r"].at[nz - dz], dev(dz, 0, 0, c))

    whole_c = slice(AT_C, AT_C + STREAM_C)

    def step_c6():
        for dz in _peers(nz):
            arrived(rows_c(dz, 0, cz), s["c5_r"].at[dz])
        share(fin.at[c, whole_c], len(STREAMS), 0)

    for i in range(nz):
        gc[(i + 1) * stride_c - SUB : (i + 1) * stride_c, :] = loss_tile
    de_all = de[...]
    e, inv = unit[0, :, :L], unit[0, :, L:]
    dz_h = (inv * (de_all - e * jnp.sum(e * de_all, axis=1, keepdims=True))).astype(BF16)
    put(AT_3, _dot(acts[0, H2_AT:ACT_ROWS, :], dz_h))
    da2 = jnp.where(hid[0, :, W_A:] > 0, _dot(dz_h, s["w3"][c], NT), 0.0).astype(BF16)
    dw2 = _dot(acts[0, H1_AT:H2_AT, :], da2)
    for j in range(COLS):
        put(AT_2 + W_A * j, dw2[:, _lanes(j)])
    phase1(sets[0])
    step_c1()
    da1 = jnp.where(hid[0, :, :W_A] > 0, _dot(da2, s["w2"][c], NT), 0.0).astype(BF16)
    dw1 = _dot(acts[0, X_AT:H1_AT, :], da1)
    for j in range(COLS):
        put(AT_1 + W_IN * j, dw1[:, _lanes(j)])
    phase1(sets[1])

    for name, steps in (
        ("ar2", (phase2, phase2, step_c2)),
        ("ar3", (phase3, step_c3, phase3)),
        ("ar4", (phase4, step_c4, phase4)),
        ("ar5", (phase5, step_c5, phase5)),
        ("ar6", (phase6, phase6)),
        ("ar7", (step_c6, phase7, phase7)),
    ):
        n = 0
        for i, step in enumerate(steps):
            mark(f"{name}_{i}")
            if step in (phase2, phase6, phase7):
                step(sets[n])
                n += 1
            elif step in (phase3, phase4, phase5):
                step(n, sets[n])
                n += 1
            else:
                step()
    mark("sib_wait")
    arrived(lossb.at[1 - c], s["ls_r"])
    loss[...] = jnp.sum(lossb[0] + lossb[1], axis=1, keepdims=True)[:1] * inv_batch + jnp.zeros(loss.shape, F32)
    for pair in sets:
        for st in pair:
            for d in range(st.n1):
                arrived(fin.at[1 - c, st.chunk1(d)], s["sb_r"].at[st.i, d])
    arrived(fin.at[1 - c, whole_c], s["sb_r"].at[len(STREAMS), 0])

    mark("final_waits")
    for i, (ref, n) in enumerate(((idb, n_small), (lqb, n_small), (idq, nz - 1))):
        if n:
            pltpu.make_async_copy(ref.at[pl.ds(0, n)], ref.at[pl.ds(0, n)], sm_s.at[i]).wait()

    for cp in sends:
        cp.wait_send()
    mark()


def _layout_kernel(fin, loss_in, *refs):
    outs, sem = refs[:-1], refs[-1]
    copies = []

    def put(src, dst):
        cp = pltpu.make_async_copy(src, dst, sem.at[len(copies)])
        cp.start()
        copies.append(cp)

    for t in PAIR:
        o1, o2, o3 = outs[COLS * t : COLS * (t + 1)]
        for j in range(COLS):
            put(fin.at[t, AT_1 + W_IN * j : AT_1 + W_IN * (j + 1)], o1.at[:, _lanes(j)])
            put(fin.at[t, AT_2 + W_A * j : AT_2 + W_A * (j + 1)], o2.at[:, _lanes(j)])
        put(fin.at[t, AT_3:AT_2], o3)
    outs[-1][0, 0] = jnp.max(loss_in[...])
    for cp in copies:
        cp.wait()


def _step(p, ux, ix, ids, lq, uw1, uw2, uw3, iw1, iw2, iw3):
    scratch = _scratch(p)
    anywhere, vmem = pl.BlockSpec(memory_space=pl.ANY), pl.BlockSpec(memory_space=pltpu.VMEM)
    fin, loss = pl.pallas_call(
        functools.partial(_kernel, p, tuple(scratch)),
        out_shape=(pltpu.VMEM((2, GRAD_ROWS, L), F32), pltpu.VMEM((SUB, L), F32)),
        in_specs=[anywhere] * len((ux, ix, ids, lq, uw1, uw2, uw3, iw1, iw2, iw3)),
        out_specs=(vmem, vmem),
        scratch_shapes=list(scratch.values()),
        compiler_params=pltpu.CompilerParams(collective_id=0, has_side_effects=True, vmem_limit_bytes=VMEM_BYTES),
        name="two_tower_step",
    )(ux, ix, ids.reshape(1, L), lq.reshape(1, L), uw1, uw2, uw3, iw1, iw2, iw3)
    shapes = [(W_IN, W_A), (W_A, W_B), (W_B, L)] * 2
    *grads, loss = pl.pallas_call(
        _layout_kernel,
        out_shape=[jax.ShapeDtypeStruct(a, F32) for a in [*shapes, (1, 1)]],
        in_specs=[vmem, vmem],
        out_specs=[anywhere] * len(shapes) + [pl.BlockSpec(memory_space=pltpu.SMEM)],
        scratch_shapes=[pltpu.SemaphoreType.DMA((2 * (2 * COLS + 1),))],
        compiler_params=pltpu.CompilerParams(vmem_limit_bytes=LAYOUT_BYTES),
        name="layout",
    )(fin, loss)
    return (loss.reshape(()), *grads)


def solution(mesh):
    p = _Plan(mesh.shape["dp"])
    rows, vec, whole = P("dp", None), P("dp"), P()
    return jax.shard_map(
        functools.partial(_step, p),
        mesh=mesh,
        in_specs=(rows, rows, vec, vec, whole, whole, whole, whole, whole, whole),
        out_specs=(whole,) * (1 + 2 * COLS),
        check_vma=False,
    )
```

```python
import functools
import math

import jax
import jax.numpy as jnp
from jax import lax
from jax.experimental import pallas as pl
from jax.experimental.pallas import tpu as pltpu
from jax.sharding import PartitionSpec as P

F32, BF16, I32 = jnp.float32, jnp.bfloat16, jnp.int32
MESH = pl.DeviceIdType.MESH

GRID = {256: (8, 4, 4)}

L, SUB = 128, 8
PAIR = range(2)
USER, ITEM = PAIR
W_IN, W_A, W_B = 256, 384, 384
DUO = 2 * L
MAX_GROUPS = 32
TEMP = 0.05
INV_TEMP = 1.0 / TEMP
EXP_SCALE = INV_TEMP * math.log2(math.e)
NORM_EPS = 1e-6
LOW = -3.0e38
ROWS_1, ROWS_2, ROWS_3 = W_IN * W_A // L, W_A * W_B // L, W_B
AT_3, AT_2, AT_1 = 0, ROWS_3, ROWS_3 + ROWS_2
GRAD_ROWS = AT_1 + ROWS_1
STREAM, STREAM_C = 512, 256
AT_C = 2 * STREAM
STREAMS = (0, STREAM, AT_C + STREAM_C, AT_C + STREAM_C + STREAM)
COLS = W_A // L
X_AT, H1_AT, H2_AT, ACT_ROWS = 0, W_IN, W_IN + W_A, W_IN + W_A + W_B
GROUP = 4
LAG = 1
VMEM_BYTES, LAYOUT_BYTES = 56 << 20, 1 << 20
NN = (((1,), (0,)), ((), ()))
NT = (((1,), (1,)), ((), ()))


def _dot(a, b, dims=NN):
    return lax.dot_general(a, b, dims, preferred_element_type=F32)


def _near(k):
    return k + k // 2 - 2 * (k // 3)


def _lanes(j, n=1):
    return slice(j * L, (j + n) * L)


def _at(start, size):
    return pl.ds(pl.multiple_of(start, SUB), size)


def _peers(n):
    return range(1, n)


def _iota(shape, dim):
    return lax.broadcasted_iota(I32, shape, dim)


class _Marks:
    def __init__(self):
        self.scope = None

    def __call__(self, name=None):
        if self.scope is not None:
            self.scope.__exit__(None, None, None)
        self.scope = jax.named_scope(name) if name else None
        if name:
            self.scope.__enter__()


class _Plan:
    def __init__(self, n):
        nz, ny, nx = self.nz, self.ny, self.nx = GRID[n]
        self.plane = nx * ny
        self.batch = n * L
        self.queries = nz * L
        self.ch1 = tuple(STREAM // m for m in (nx, ny))
        self.ch2 = STREAM // self.plane
        self.zc = 2 * self.ch2 // nz
        self.cz = STREAM_C // nz
        self.cx = self.cz // nx
        self.offsets = [(_near(k // nx), _near(k % nx)) for k in range(self.plane)]
        self.evens = sorted(range(0, nz, 2), key=lambda d: -min(d, nz - d))

    def slot(self, dy, dx):
        return self.offsets.index((dy % self.ny, dx % self.nx))


def _scratch(p):
    npl, nz, nq = p.plane, p.nz, p.queries
    vm, dma = pltpu.VMEM, pltpu.SemaphoreType.DMA
    groups, most = 2 * npl, max(p.nx, p.ny)
    chunk = max(p.ch1)
    items = npl * DUO
    return dict(
        xs=vm((2, L, W_IN), F32),
        wf1=vm((2, W_IN, W_A), F32),
        wf2=vm((2, W_A, W_B), F32),
        wf3=vm((2, W_B, L), F32),
        w2=vm((2, W_A, W_B), BF16),
        w3=vm((2, W_B, L), BF16),
        acts=vm((2, ACT_ROWS, DUO), BF16),
        hid=vm((2, DUO, W_A + W_B), BF16),
        unit=vm((2, DUO, DUO), F32),
        ids0=vm((1, L), I32),
        lq0=vm((1, L), F32),
        inf=vm((groups, 4, L), F32),
        qinf=vm((nz, 4, L), F32),
        lqk=vm((MAX_GROUPS, L), F32),
        hik=vm((MAX_GROUPS, L), F32),
        lok=vm((MAX_GROUPS, L), F32),
        idc=vm((items, L), I32),
        vaug=vm((items, DUO), BF16),
        vt=vm((L, items), BF16),
        uall=vm((nq, L), BF16),
        ut=vm((DUO, nq), BF16),
        tb=vm((items, nq), F32),
        ls=vm((SUB, nq), F32),
        dg=vm((1, L), F32),
        lse=vm((2, nq), F32),
        stat=vm((2, nz, 2, nq // 2), F32),
        fac=vm((2, nq), F32),
        gt=vm((items, nq), BF16),
        dvp=vm((npl * 2, L, L), F32),
        dvs=vm((npl, L, L), F32),
        dvo=vm((npl, L, L), F32),
        dut=vm((nz, L, L), F32),
        rx=vm((2 * nz, L, L), F32),
        xya=vm((2, most, most, L // 2, L), F32),
        xyb=vm((2, most, L // 2, L), F32),
        rv=vm((2, most, 2, L // 2, L), F32),
        de=vm((DUO, L), F32),
        g=vm((GRAD_ROWS, L), F32),
        gc=vm((nz * (p.cz + SUB), L), F32),
        r1=vm((4, most, chunk, L), F32),
        s1=vm((4, chunk, L), F32),
        r2=vm((4, most, p.ch2, L), F32),
        s2=vm((2, 2 * p.ch2, L), F32),
        r3=vm((2, nz, p.zc, L), F32),
        rc1=vm((nz, p.cz + SUB, L), F32),
        sc1=vm((p.cz + SUB, L), F32),
        rc2=vm((p.nx, p.cx + SUB, L), F32),
        rc3=vm((p.ny, p.cx + SUB, L), F32),
        lossb=vm((2, SUB, L), F32),
        ld=dma((2 + 2 * 4,)),
        sm_s=dma((2,)),
        sm_r=dma((2,)),
        v_s=dma((npl,)),
        v_r=dma((npl,)),
        fw_s=dma((npl,)),
        fw_r=dma((npl,)),
        u_s=dma((nz,)),
        u_r=dma((nz,)),
        ac_s=dma((3,)),
        ac_r=dma((3,)),
        st_s=dma((2, nz)),
        st_r=dma((2, nz)),
        dv_s=dma((npl,)),
        dv_r=dma((npl,)),
        xy_s=dma((2, most, most)),
        xy_r=dma((2, most, most)),
        rv_s=dma((2, most)),
        rv_r=dma((2, most, 2)),
        du_s=dma((nz,)),
        rx_r=dma((2 * nz,)),
        p1_s=dma((4, most)),
        p1_r=dma((4, most)),
        p2_s=dma((4, most)),
        p2_r=dma((4, most)),
        p3_s=dma((2, nz)),
        p3_r=dma((2, nz)),
        p4_s=dma((2, nz)),
        p4_r=dma((2, nz)),
        p5_s=dma((4, most)),
        p5_r=dma((4, most)),
        p6_s=dma((4, most)),
        p6_r=dma((4, most)),
        sb_s=dma((4 + 1, most)),
        sb_r=dma((4 + 1, most)),
        c1_s=dma((nz,)),
        c1_r=dma((nz,)),
        c2_s=dma((2, p.nx)),
        c2_r=dma((2, p.nx)),
        c3_s=dma((p.ny,)),
        c3_r=dma((p.ny,)),
        c4_s=dma((p.nx,)),
        c4_r=dma((p.nx,)),
        c5_s=dma((nz,)),
        c5_r=dma((nz,)),
        ls_s=dma(()),
        ls_r=dma(()),
    )


def _kernel(p, names, ux, ix, ids, lq, uw1, uw2, uw3, iw1, iw2, iw3, fin, loss, *refs):
    s = dict(zip(names, refs, strict=True))
    nz, ny, nx, npl, nq = p.nz, p.ny, p.nx, p.plane, p.queries
    half = nz // 2
    mark = _Marks()
    me = lax.axis_index("dp")
    c = lax.rem(me, 2)
    chip = lax.div(me, 2)
    x = lax.rem(chip, nx)
    y = lax.rem(lax.div(chip, nx), ny)
    z = lax.div(chip, nx * ny)
    sibling = me + 1 - 2 * c

    def dev(dz, dy, dx, core):
        zz, yy, xx = lax.rem(z + dz, nz), lax.rem(y + dy, ny), lax.rem(x + dx, nx)
        return ((zz * ny + yy) * nx + xx) * 2 + core

    def rcopy(src, dst, send, recv, to):
        return pltpu.make_async_remote_copy(
            src_ref=src, dst_ref=dst, send_sem=send, recv_sem=recv, device_id=(to,), device_id_type=MESH
        )

    sends = []

    def send(src, dst, ssem, rsem, to):
        cp = rcopy(src, dst, ssem, rsem, to)
        cp.start()
        sends.append(cp)

    def arrived(dst, rsem):
        rcopy(dst, dst, rsem, rsem, me).wait_recv()

    lane = pl.ds(pl.multiple_of(c * L, L), L)
    other = pl.ds(pl.multiple_of((1 - c) * L, L), L)

    mark("start")
    xs, inf, qinf, ld = s["xs"], s["inf"], s["qinf"], s["ld"]
    small = [pltpu.make_async_copy(a, s[b], ld.at[i]) for i, (a, b) in enumerate(((ids, "ids0"), (lq, "lq0")))]
    loads = {}
    n_ld = len(small)
    for t, given in ((ITEM, (ix, iw1, iw2, iw3)), (USER, (ux, uw1, uw2, uw3))):
        loads[t] = []
        for src, dst in zip(given, (xs, s["wf1"], s["wf2"], s["wf3"]), strict=True):
            loads[t].append(pltpu.make_async_copy(src, dst.at[t], ld.at[n_ld]))
            n_ld += 1
    for cp in small + loads[ITEM] + loads[USER]:
        cp.start()

    barrier = pltpu.get_barrier_semaphore()
    others = [dev(0, dy, dx, core) for core in PAIR for dy, dx in p.offsets[1:]]
    others += [dev(dz, 0, 0, core) for core in PAIR for dz in _peers(nz)]
    others.append(sibling)
    for to in others:
        pl.semaphore_signal(barrier, inc=1, device_id=(to,), device_id_type=MESH)

    acts, hid, unit = s["acts"], s["hid"], s["unit"]

    def tower(t):
        place = jnp.where(c == t, 0, 1)
        for cp in loads[t]:
            cp.wait()
        w1, w2, w3 = s["wf1"][t].astype(BF16), s["wf2"][t].astype(BF16), s["wf3"][t].astype(BF16)
        s["w2"][t], s["w3"][t] = w2, w3
        xh = xs[t].astype(BF16)
        h1 = jnp.maximum(_dot(xh, w1), 0.0).astype(BF16)
        h2 = jnp.maximum(_dot(h1, w2), 0.0).astype(BF16)
        raw = _dot(h2, w3)
        inv = lax.rsqrt(jnp.sum(raw * raw, axis=1, keepdims=True) + NORM_EPS)
        e = raw * inv
        acts[place, X_AT:H1_AT, lane] = xh.T
        acts[place, H1_AT:H2_AT, lane] = h1.T
        acts[place, H2_AT:ACT_ROWS, lane] = h2.T
        hid[place, lane, :W_A] = h1
        hid[place, lane, W_A:] = h2
        unit[place, lane, :L] = e
        unit[place, lane, L:] = jnp.broadcast_to(inv, (L, L))
        return e.astype(BF16)

    mark("towers")
    vaug, uall = s["vaug"], s["uall"]

    def tile_of(zz):
        return lax.div(zz, 2) + lax.rem(zz, 2) * half

    def z_of(r):
        return 2 * (r % half) + r // half

    mine = tile_of(z)
    vaug[lane, :L] = tower(ITEM)
    uall[pl.ds(pl.multiple_of(mine * L, L), L), :] = tower(USER)
    for cp in small:
        cp.wait()
    word = 1 << 16
    id_own, lq_own = s["ids0"][...], s["lq0"][...]
    told = jnp.concatenate(
        [lq_own, (id_own // word).astype(F32), (id_own % word).astype(F32), jnp.zeros((1, L), F32)], axis=0
    )
    inf[c] = told
    qinf[mine] = told
    mark("barrier_wait")
    pl.semaphore_wait(barrier, len(others))

    mark("send_uv")
    sm_s, sm_r = s["sm_s"], s["sm_r"]

    def send_small(k, to):
        rcopy(inf.at[c], inf.at[2 * k + c], sm_s.at[0], sm_r.at[0], to).start()

    for dy, dx in p.offsets[1:]:
        for core in PAIR:
            send_small(p.slot(-dy, -dx), dev(0, dy, dx, core))
    send_small(0, sibling)
    n_small = 2 * npl - 1
    for dz in _peers(nz):
        rcopy(qinf.at[mine], qinf.at[mine], sm_s.at[1], sm_r.at[1], dev(dz, 0, 0, c)).start()
    small_waits = ((inf, n_small), (qinf, nz - 1))

    def vpart(k, core):
        return vaug.at[pl.ds(pl.multiple_of(k * DUO + core * L, L), L), pl.ds(0, L)]

    def upart(j):
        return uall.at[pl.ds(pl.multiple_of(j * L, L), L)]

    send(vpart(0, c), vpart(0, c), s["fw_s"].at[0], s["fw_r"].at[0], sibling)
    z_near = sorted(_peers(nz), key=lambda d: min(d, nz - d))
    for i in range(max(npl, nz) - 1):
        if i < nz - 1:
            dz = z_near[i]
            send(upart(mine), upart(mine), s["u_s"].at[dz], s["u_r"].at[nz - dz], dev(dz, 0, 0, c))
        if i + 1 < npl:
            dy, dx = p.offsets[i + 1]
            k = p.slot(-dy, -dx)
            send(vpart(0, c), vpart(k, c), s["v_s"].at[i + 1], s["v_r"].at[k], dev(0, dy, dx, c))
    for i, part in enumerate(((acts, slice(None), lane), (hid, lane, slice(None)), (unit, lane, slice(None)))):
        ref, rows, cols = part
        send(ref.at[1, rows, cols], ref.at[0, rows, cols], s["ac_s"].at[i], s["ac_r"].at[i], sibling)

    mark("small_wait")
    lqk, hik, lok, idc, ut = s["lqk"], s["hik"], s["lok"], s["idc"], s["ut"]
    lqk[...] = jnp.full(lqk.shape, -LOW, F32)
    hik[...] = jnp.full(hik.shape, -1.0, F32)
    lok[...] = jnp.full(lok.shape, -1.0, F32)
    ut[L:, :] = jnp.where(_iota((L, nq), 0) < 3 * MAX_GROUPS, -1.0, 0.0).astype(BF16)
    for i, (ref, n) in enumerate(small_waits):
        if n:
            pltpu.make_async_copy(ref.at[pl.ds(0, n)], ref.at[pl.ds(0, n)], sm_r.at[i]).wait()
    mark("turn")

    def ident(hi, lo):
        return hi.astype(I32) * word + lo.astype(I32)

    for g in range(2 * npl):
        hi, lo = inf[g, 1:2, :], inf[g, 2:3, :]
        lqk[g : g + 1, :] = inf[g, :1, :] * TEMP
        hik[g : g + 1, :] = hi
        lok[g : g + 1, :] = lo
        idc[_lanes(g), :] = jnp.broadcast_to(ident(hi, lo), (L, L)).T
    idq = [ident(qinf[r, 1:2, :], qinf[r, 2:3, :]) for r in range(nz)]

    def parts(q):
        hi = q.astype(BF16).astype(F32)
        mid = (q - hi).astype(BF16).astype(F32)
        return hi, mid, (q - hi - mid).astype(BF16).astype(F32)

    q_all, id_hi, id_lo = lqk[...], hik[...], lok[...]
    split = parts(jnp.where(id_hi < 0.0, 0.0, q_all))
    turned = jnp.concatenate([*split, jnp.zeros((MAX_GROUPS, L), F32)], axis=0).T.astype(BF16)
    col = _iota((L, L), 1)
    ones = jnp.where(col < 3 * MAX_GROUPS + 3, 1.0, 0.0)
    for g in range(2 * npl):
        keep = jnp.where(col < 3 * MAX_GROUPS, jnp.where(lax.rem(col, MAX_GROUPS) == g, turned.astype(F32), 0.0), ones)
        vaug[_lanes(g), L:] = keep.astype(BF16)

    def most(a):
        return jnp.max(jnp.max(a, axis=0, keepdims=True), axis=1, keepdims=True)

    top1 = most(-q_all)
    at_top = -q_all == top1
    top_hi = most(jnp.where(at_top, id_hi, -1.0))
    top_lo = most(jnp.where(jnp.logical_and(at_top, id_hi == top_hi), id_lo, -1.0))
    same_top = jnp.logical_and(id_hi == top_hi, id_lo == top_lo)
    top2 = most(jnp.where(same_top, LOW, -q_all))
    top2 = jnp.where(top2 <= LOW, top1, top2)
    id_top = ident(top_hi, top_lo)
    stat = s["stat"]
    bounds = []
    for r in range(nz):
        rest = jnp.maximum(top2, jnp.where(z == z_of(r), -lq_own * TEMP, LOW))
        bounds.append(jnp.where(idq[r] == id_top, rest, jnp.broadcast_to(top1, (1, L))))
    bound = jnp.concatenate(bounds, axis=1)
    ends = (range(half), range(half, nz))
    for h in PAIR:
        stat[h, 0, :1, :] = jnp.concatenate([bounds[r] for r in ends[h]], axis=1)
    at = L + 3 * MAX_GROUPS
    ut[at : at + 16, :] = jnp.concatenate([-a for a in parts(bound)] + [jnp.zeros((16 - 3, nq), F32)], axis=0).astype(BF16)

    mark("u_wait")
    tb, ls, vt, dg = s["tb"], s["ls"], s["vt"], s["dg"]
    dg[...] = jnp.zeros(dg.shape, F32)
    for dz in z_near:
        arrived(upart(tile_of(lax.rem(z + dz, nz))), s["u_r"].at[dz])
    for r in range(nz):
        ut[:L, _lanes(r)] = uall[_lanes(r), :].T
    item_row, query_at = _iota((DUO, L), 0), _iota((DUO, L), 1) + c * L

    def is_diag(r):
        return item_row == query_at + jnp.where(z == z_of(r), 0, DUO)

    def pass1(blocks, tiles):
        rows = slice(blocks[0] * DUO, (blocks[-1] + 1) * DUO)
        wide = _dot(vaug[rows, :], ut[:, _lanes(tiles[0], len(tiles))])
        for i, r in enumerate(tiles):
            add = 0.0
            for n, k in enumerate(blocks):
                at = slice(k * DUO, (k + 1) * DUO)
                t = wide[n * DUO : (n + 1) * DUO, _lanes(i)]
                drop = idc[at, :] == idq[r]
                if k == 0:
                    pair = is_diag(r)
                    drop = jnp.logical_and(drop, jnp.logical_not(pair))
                    dg[...] += jnp.sum(jnp.where(pair, t, 0.0), axis=0, keepdims=True)
                e = jnp.where(drop, 0.0, jnp.exp2(t * EXP_SCALE))
                tb[at, _lanes(r)] = e
                add = add + jnp.sum(e.reshape(DUO // SUB, SUB, L), axis=0)
            if blocks[0] == 0:
                ls[:, _lanes(r)] = add
            else:
                ls[:, _lanes(r)] += add

    def forward(blocks):
        for k in blocks:
            if k:
                arrived(vpart(k, c), s["v_r"].at[k])
                send(vpart(k, c), vpart(k, c), s["fw_s"].at[k], s["fw_r"].at[k], sibling)

    def send_stats(h):
        cols = _lanes(h * half, half)
        stat[h, 0, 1:, :] = jnp.sum(ls[:, cols], axis=0, keepdims=True)
        for dz in _peers(nz):
            send(stat.at[h, 0], stat.at[h, nz - dz], s["st_s"].at[h, dz], s["st_r"].at[h, nz - dz], dev(dz, 0, 0, c))

    size = min(GROUP, npl)
    groups = [range(a, a + size) for a in range(0, npl, size)]
    mark("pass1a")
    forward(groups[0])
    for n, blocks in enumerate(groups):
        if n + 1 < len(groups):
            forward(groups[n + 1])
        for k in blocks:
            arrived(vpart(k, 1 - c), s["fw_r"].at[k])
        pass1(blocks, ends[0])
    send_stats(0)
    mark("pass1b")
    for blocks in groups:
        pass1(blocks, ends[1])
    send_stats(1)
    mark("flip")
    for k in range(2 * npl):
        vt[:, _lanes(k)] = vaug[_lanes(k), :L].T

    fac, lse = s["fac"], s["lse"]
    inv_batch = 1.0 / p.batch

    def statistics(h):
        cols = _lanes(h * half, half)
        for dz in _peers(nz):
            arrived(stat.at[h, dz], s["st_r"].at[h, dz])
        sums = [stat[h, dz, 1:, :] for dz in range(nz)]
        tops = [jnp.where(a > 0.0, stat[h, dz, :1, :], LOW) for dz, a in enumerate(sums)]
        top = functools.reduce(jnp.maximum, tops)
        total = sum(a * jnp.exp2((b - top) * EXP_SCALE) for a, b in zip(sums, tops, strict=True))
        fac[:1, cols] = jnp.exp2((tops[0] - top) * EXP_SCALE) * (1.0 / total)
        fac[1:, cols] = fac[:1, cols] * inv_batch
        lse[:1, cols] = top - bound[:, cols]
        lse[1:, cols] = total

    gt, dut, dvp, dvs, dvo, rx = s["gt"], s["dut"], s["dvp"], s["dvs"], s["dvo"], s["rx"]

    def grads(blocks, tiles):
        for k in blocks:
            at = slice(k * DUO, (k + 1) * DUO)
            for r in tiles:
                if k == 0:
                    g = (tb[at, _lanes(r)] * fac[:1, _lanes(r)] - jnp.where(is_diag(r), 1.0, 0.0)) * inv_batch
                else:
                    g = tb[at, _lanes(r)] * fac[1:, _lanes(r)]
                gt[at, _lanes(r)] = g.astype(BF16)

    def user_part(blocks, tiles, first):
        rows = slice(blocks[0] * DUO, (blocks[-1] + 1) * DUO)
        part = _dot(vt[:, rows], gt[rows, _lanes(tiles[0], len(tiles))])
        for i, r in enumerate(tiles):
            piece = part[:, _lanes(i)]
            dut[r] = piece if first else dut[r] + piece

    def item_part(blocks):
        rows = slice(blocks[0] * DUO, (blocks[-1] + 1) * DUO)
        part = _dot(ut[:L, :], gt[rows, :], NT)
        for i in range(2 * len(blocks)):
            dvp[2 * blocks[0] + i] = part[:, _lanes(i)]

    def give_sibling(blocks):
        for k in reversed(blocks):
            send(dvp.at[2 * k + 1 - c], dvs.at[k], s["dv_s"].at[k], s["dv_r"].at[k], sibling)

    guarded = []

    def send_du(h):
        for i, d in enumerate(p.evens):
            zz = lax.rem(z + d + lax.rem(h + z, 2), nz)
            to = ((zz * ny + y) * nx + x) * 2
            cp = rcopy(
                dut.at[tile_of(zz)], rx.at[2 * z + c], s["du_s"].at[h * half + i], s["rx_r"].at[2 * z + c], to
            )
            pl.when(to != me)(cp.start)
            guarded.append((to != me, cp))

    top_rows, low_rows = pl.ds(0, L // 2), pl.ds(L // 2, L // 2)
    xya, xyb, rv = s["xya"], s["xyb"], s["rv"]

    def finish(blocks):
        for k in reversed(blocks):
            arrived(dvs.at[k], s["dv_r"].at[k])
            dvo[k] = dvp[2 * k + c] + dvs[k]
            dy, dx = p.offsets[k]
            for part, rows, d, rest, n, to in (
                (0, top_rows, dx, dy, nx, (0, dx)),
                (1, low_rows, dy, dx, ny, (dy, 0)),
            ):
                if d:
                    sem = (part, n - d, rest)
                    send(dvo.at[k, rows], xya.at[sem], s["xy_s"].at[sem], s["xy_r"].at[sem], dev(0, *to, c))

    def second_step(part, d):
        n = ny if part else nx
        k = p.offsets.index((0, d) if part else (d, 0))
        acc = dvo[k, low_rows if part else top_rows, :]
        for i in reversed(_peers(n)):
            arrived(xya.at[part, i, d], s["xy_r"].at[part, i, d])
            acc = acc + xya[part, i, d]
        m = nx if part else ny
        if d:
            xyb[part, d] = acc
            to = dev(0, 0, d, 1) if part else dev(0, d, 0, 1)
            send(xyb.at[part, d], rv.at[part, m - d, c], s["rv_s"].at[part, d], s["rv_r"].at[part, m - d, c], to)
        else:
            rv[part, 0, c] = acc

    mark("stat_a")
    statistics(0)
    mark("pass2a")
    grads(groups[0], ends[0])
    for n, blocks in enumerate(groups):
        user_part(blocks, ends[0], n == 0)
        if n + 1 < len(groups):
            grads(groups[n + 1], ends[0])
    send_du(0)
    mark("stat_b")
    statistics(1)
    mark("pass2b")
    grads(groups[0], ends[1])
    for n, blocks in enumerate(groups):
        user_part(blocks, ends[1], n == 0)
        if n + 1 < len(groups):
            grads(groups[n + 1], ends[1])
    send_du(1)
    mark("pass2c")
    order, lo = [], npl
    while lo:
        take = min(GROUP if len(order) > 1 else GROUP // 2, lo)
        order.append(range(lo - take, lo))
        lo -= take
    for n, blocks in enumerate(order):
        item_part(blocks)
        give_sibling(blocks)
        if n >= LAG:
            finish(order[n - LAG])
    mark("rs_first")
    for blocks in order[-LAG:]:
        finish(blocks)
    mark("rs_second")
    for i in reversed(range(max(nx, ny))):
        for part in PAIR:
            d = _near(i)
            if d < (nx if part else ny):
                second_step(part, d)
    own_cols = pl.ds(pl.multiple_of(mine * L, L), L)
    loss_part = (lse[:1, own_cols] - dg[...]) * INV_TEMP + jnp.log(lse[1:, own_cols])
    loss_tile = jnp.where(_iota((SUB, L), 0) == 0, loss_part, 0.0)

    mark("rs_wait")
    de = s["de"]

    def gather(h, acc, order):
        for j in order:
            arrived(rx.at[j], s["rx_r"].at[j])
            acc = rx[j] if acc is None else acc + rx[j]
        de[_lanes(h), :] = acc.T * INV_TEMP

    z_from = [lax.rem(z + d, nz) for d in reversed(z_near)]

    @pl.when(c == USER)
    def _():
        cps = []
        for part in PAIR:
            cps.append(rcopy(rv.at[part, 0, 0], rv.at[part, 0, 0], s["rv_s"].at[part, 0], s["rv_r"].at[part, 0, 0], sibling))
            cps[-1].start()
        gather(0, dut[mine], [2 * a for a in z_from])
        gather(1, None, [2 * a + 1 for a in [*z_from, z]])
        for cp in cps:
            cp.wait_send()

    @pl.when(c == ITEM)
    def _():
        for h in reversed(PAIR):
            sums = []
            for part in PAIR:
                acc = None
                for d in [*reversed(_peers(nx if part else ny)), 0]:
                    if d or h == 0:
                        arrived(rv.at[part, d, h], s["rv_r"].at[part, d, h])
                    acc = rv[part, d, h] if acc is None else acc + rv[part, d, h]
                sums.append(acc)
            de[_lanes(h), :] = jnp.concatenate(sums, axis=0).T * INV_TEMP

    mark("backward")
    arrived(acts.at[0, :, other], s["ac_r"].at[0])
    arrived(hid.at[0, other, :], s["ac_r"].at[1])
    arrived(unit.at[0, other, :], s["ac_r"].at[2])
    g, gc = s["g"], s["gc"]
    cz, cx, ch2, zc = p.cz, p.cx, p.ch2, p.zc
    stride_c = cz + SUB

    def put(start, val):
        n, done = val.shape[0], 0
        while done < n:
            row = start + done
            if AT_C <= row < AT_C + STREAM_C:
                chunk, off = (row - AT_C) // cz, (row - AT_C) % cz
                take = min(n - done, cz - off)
                to = chunk * stride_c + off
                gc[to : to + take, :] = val[done : done + take]
            else:
                take = n - done if row >= AT_C else min(n - done, AT_C - row)
                g[row : row + take, :] = val[done : done + take]
            done += take

    def toward(along_x, d):
        return dev(0, 0, d, c) if along_x else dev(0, d, 0, c)

    class Stream:
        def __init__(self, i):
            self.i, self.start = i, STREAMS[i]
            self.along_x = i % 2 == 0
            self.n1, self.n2 = (nx, ny) if self.along_x else (ny, nx)
            self.q1, self.q2 = (x, y) if self.along_x else (y, x)
            self.ch1 = STREAM // self.n1

        def to1(self, d):
            return toward(self.along_x, d)

        def to2(self, d):
            return toward(not self.along_x, d)

        def chunk1(self, d):
            return _at(self.start + lax.rem(self.q1 + d, self.n1) * self.ch1, self.ch1)

        def row2(self, d):
            return self.start + self.q1 * self.ch1 + lax.rem(self.q2 + d, self.n2) * ch2

        def sem(self, name, d):
            return s[name].at[self.i, d]

    streams = [Stream(i) for i in range(len(STREAMS))]
    sets = (streams[:2], streams[2:])
    r1, s1, r2, s2, r3, lossb = s["r1"], s["s1"], s["r2"], s["s2"], s["r3"], s["lossb"]
    rc1, sc1, rc2, rc3 = s["rc1"], s["sc1"], s["rc2"], s["rc3"]

    def phase1(pair):
        for d in _peers(max(nx, ny)):
            for st in pair:
                if d < st.n1:
                    send(g.at[st.chunk1(d)], r1.at[st.i, d, : st.ch1], st.sem("p1_s", d), st.sem("p1_r", d), st.to1(d))

    def phase2(pair):
        for st in pair:
            acc = g[st.chunk1(0), :]
            for d in _peers(st.n1):
                arrived(r1.at[st.i, d, : st.ch1], st.sem("p1_r", d))
                acc = acc + r1[st.i, d, : st.ch1, :]
            s1[st.i, : st.ch1, :] = acc
            for d in _peers(st.n2):
                at = _at(lax.rem(st.q2 + d, st.n2) * ch2, ch2)
                send(s1.at[st.i, at], r2.at[st.i, d], st.sem("p2_s", d), st.sem("p2_r", d), st.to2(d))

    def phase3(n, pair):
        for j, st in enumerate(pair):
            acc = s1[st.i, _at(st.q2 * ch2, ch2), :]
            for d in _peers(st.n2):
                arrived(r2.at[st.i, d], st.sem("p2_r", d))
                acc = acc + r2[st.i, d]
            s2[n, j * ch2 : (j + 1) * ch2, :] = acc
        for dz in _peers(nz):
            at = _at(lax.rem(z + dz, nz) * zc, zc)
            send(s2.at[n, at], r3.at[n, dz], s["p3_s"].at[n, dz], s["p3_r"].at[n, dz], dev(dz, 0, 0, c))

    def place(pair, dz):
        zz = lax.rem(z + dz, nz)
        second = lax.div(zz, nz // 2)
        first = pair[0].row2(0) * (1 - second) + pair[1].row2(0) * second
        return fin.at[c, _at(first + lax.rem(zz, nz // 2) * zc, zc)]

    def phase4(n, pair):
        acc = s2[n, _at(z * zc, zc), :]
        for dz in _peers(nz):
            arrived(r3.at[n, dz], s["p3_r"].at[n, dz])
            acc = acc + r3[n, dz]
        place(pair, 0)[...] = acc
        for dz in _peers(nz):
            send(place(pair, 0), place(pair, 0), s["p4_s"].at[n, dz], s["p4_r"].at[n, nz - dz], dev(dz, 0, 0, c))

    def phase5(n, pair):
        for dz in _peers(nz):
            arrived(place(pair, dz), s["p4_r"].at[n, dz])
        for st in pair:
            rows = fin.at[c, _at(st.row2(0), ch2)]
            for d in _peers(st.n2):
                send(rows, rows, st.sem("p5_s", d), st.sem("p5_r", st.n2 - d), st.to2(d))

    def share(rows, i, d):
        send(rows, rows, s["sb_s"].at[i, d], s["sb_r"].at[i, d], sibling)

    def phase6(pair):
        for st in pair:
            for d in _peers(st.n2):
                arrived(fin.at[c, _at(st.row2(d), ch2)], st.sem("p5_r", d))
            rows = fin.at[c, st.chunk1(0)]
            for d in _peers(st.n1):
                send(rows, rows, st.sem("p6_s", d), st.sem("p6_r", st.n1 - d), st.to1(d))
            share(rows, st.i, 0)

    def phase7(pair):
        for d in _peers(max(nx, ny)):
            for st in pair:
                if d < st.n1:
                    rows = fin.at[c, st.chunk1(d)]
                    arrived(rows, st.sem("p6_r", d))
                    share(rows, st.i, d)

    def step_c1():
        for dz in _peers(nz):
            at = _at(lax.rem(z + dz, nz) * stride_c, stride_c)
            send(gc.at[at], rc1.at[dz], s["c1_s"].at[dz], s["c1_r"].at[dz], dev(dz, 0, 0, c))

    def step_c2():
        acc = gc[_at(z * stride_c, stride_c), :]
        for dz in _peers(nz):
            arrived(rc1.at[dz], s["c1_r"].at[dz])
            acc = acc + rc1[dz]
        sc1[...] = acc
        for d in _peers(nx):
            at, to = _at(lax.rem(x + d, nx) * cx, cx), dev(0, 0, d, c)
            send(sc1.at[at], rc2.at[d, :cx], s["c2_s"].at[0, d], s["c2_r"].at[0, d], to)
            send(sc1.at[cz:], rc2.at[d, cx:], s["c2_s"].at[1, d], s["c2_r"].at[1, d], to)

    def step_c3():
        acc, loss_acc = sc1[_at(x * cx, cx), :], sc1[cz:, :]
        for d in _peers(nx):
            arrived(rc2.at[d, :cx], s["c2_r"].at[0, d])
            arrived(rc2.at[d, cx:], s["c2_r"].at[1, d])
            acc, loss_acc = acc + rc2[d, :cx, :], loss_acc + rc2[d, cx:, :]
        rc3[y, :cx, :] = acc
        rc3[y, cx:, :] = loss_acc
        for d in _peers(ny):
            send(rc3.at[y], rc3.at[y], s["c3_s"].at[d], s["c3_r"].at[ny - d], dev(0, d, 0, c))

    def rows_c(dz, d, size):
        return fin.at[c, _at(AT_C + lax.rem(z + dz, nz) * cz + lax.rem(x + d, nx) * (cx if size == cx else 0), size)]

    def step_c4():
        for d in _peers(ny):
            arrived(rc3.at[lax.rem(y + d, ny)], s["c3_r"].at[d])
        acc = rc3[0]
        for d in _peers(ny):
            acc = acc + rc3[d]
        rows = rows_c(0, 0, cx)
        rows[...] = acc[:cx]
        lossb[c] = acc[cx:]
        send(lossb.at[c], lossb.at[c], s["ls_s"], s["ls_r"], sibling)
        for d in _peers(nx):
            send(rows, rows, s["c4_s"].at[d], s["c4_r"].at[nx - d], dev(0, 0, d, c))

    def step_c5():
        for d in _peers(nx):
            arrived(rows_c(0, d, cx), s["c4_r"].at[d])
        rows = rows_c(0, 0, cz)
        for dz in _peers(nz):
            send(rows, rows, s["c5_s"].at[dz], s["c5_r"].at[nz - dz], dev(dz, 0, 0, c))

    whole_c = slice(AT_C, AT_C + STREAM_C)

    def step_c6():
        for dz in _peers(nz):
            arrived(rows_c(dz, 0, cz), s["c5_r"].at[dz])
        share(fin.at[c, whole_c], len(STREAMS), 0)

    for i in range(nz):
        gc[(i + 1) * stride_c - SUB : (i + 1) * stride_c, :] = loss_tile
    de_all = de[...]
    e, inv = unit[0, :, :L], unit[0, :, L:]
    dz_h = (inv * (de_all - e * jnp.sum(e * de_all, axis=1, keepdims=True))).astype(BF16)
    put(AT_3, _dot(acts[0, H2_AT:ACT_ROWS, :], dz_h))
    da2 = jnp.where(hid[0, :, W_A:] > 0, _dot(dz_h, s["w3"][c], NT), 0.0).astype(BF16)
    dw2 = _dot(acts[0, H1_AT:H2_AT, :], da2)
    for j in range(COLS):
        put(AT_2 + W_A * j, dw2[:, _lanes(j)])
    phase1(sets[0])
    step_c1()
    da1 = jnp.where(hid[0, :, :W_A] > 0, _dot(da2, s["w2"][c], NT), 0.0).astype(BF16)
    dw1 = _dot(acts[0, X_AT:H1_AT, :], da1)
    for j in range(COLS):
        put(AT_1 + W_IN * j, dw1[:, _lanes(j)])
    phase1(sets[1])

    for name, steps in (
        ("ar2", (phase2, phase2, step_c2)),
        ("ar3", (phase3, step_c3, phase3)),
        ("ar4", (phase4, step_c4, phase4)),
        ("ar5", (phase5, step_c5, phase5)),
        ("ar6", (phase6, phase6)),
        ("ar7", (step_c6, phase7, phase7)),
    ):
        n = 0
        for i, step in enumerate(steps):
            mark(f"{name}_{i}")
            if step in (phase2, phase6, phase7):
                step(sets[n])
                n += 1
            elif step in (phase3, phase4, phase5):
                step(n, sets[n])
                n += 1
            else:
                step()
    mark("sib_wait")
    arrived(lossb.at[1 - c], s["ls_r"])
    loss[...] = jnp.sum(lossb[0] + lossb[1], axis=1, keepdims=True)[:1] * inv_batch + jnp.zeros(loss.shape, F32)
    for pair in sets:
        for st in pair:
            for d in range(st.n1):
                arrived(fin.at[1 - c, st.chunk1(d)], s["sb_r"].at[st.i, d])
    arrived(fin.at[1 - c, whole_c], s["sb_r"].at[len(STREAMS), 0])

    mark("final_waits")
    for i, (ref, n) in enumerate(small_waits):
        if n:
            pltpu.make_async_copy(ref.at[pl.ds(0, n)], ref.at[pl.ds(0, n)], sm_s.at[i]).wait()

    for cp in sends:
        cp.wait_send()
    for sent, cp in guarded:
        pl.when(sent)(cp.wait_send)
    mark()


def _layout_kernel(fin, loss_in, *refs):
    outs, sem = refs[:-1], refs[-1]
    copies = []

    def put(src, dst):
        cp = pltpu.make_async_copy(src, dst, sem.at[len(copies)])
        cp.start()
        copies.append(cp)

    for t in PAIR:
        o1, o2, o3 = outs[COLS * t : COLS * (t + 1)]
        for j in range(COLS):
            put(fin.at[t, AT_1 + W_IN * j : AT_1 + W_IN * (j + 1)], o1.at[:, _lanes(j)])
            put(fin.at[t, AT_2 + W_A * j : AT_2 + W_A * (j + 1)], o2.at[:, _lanes(j)])
        put(fin.at[t, AT_3:AT_2], o3)
    outs[-1][0, 0] = jnp.max(loss_in[...])
    for cp in copies:
        cp.wait()


def _step(p, ux, ix, ids, lq, uw1, uw2, uw3, iw1, iw2, iw3):
    scratch = _scratch(p)
    anywhere, vmem = pl.BlockSpec(memory_space=pl.ANY), pl.BlockSpec(memory_space=pltpu.VMEM)
    fin, loss = pl.pallas_call(
        functools.partial(_kernel, p, tuple(scratch)),
        out_shape=(pltpu.VMEM((2, GRAD_ROWS, L), F32), pltpu.VMEM((SUB, L), F32)),
        in_specs=[anywhere] * len((ux, ix, ids, lq, uw1, uw2, uw3, iw1, iw2, iw3)),
        out_specs=(vmem, vmem),
        scratch_shapes=list(scratch.values()),
        compiler_params=pltpu.CompilerParams(collective_id=0, has_side_effects=True, vmem_limit_bytes=VMEM_BYTES),
        name="two_tower_step",
    )(ux, ix, ids.reshape(1, L), lq.reshape(1, L), uw1, uw2, uw3, iw1, iw2, iw3)
    shapes = [(W_IN, W_A), (W_A, W_B), (W_B, L)] * 2
    *grads, loss = pl.pallas_call(
        _layout_kernel,
        out_shape=[jax.ShapeDtypeStruct(a, F32) for a in [*shapes, (1, 1)]],
        in_specs=[vmem, vmem],
        out_specs=[anywhere] * len(shapes) + [pl.BlockSpec(memory_space=pltpu.SMEM)],
        scratch_shapes=[pltpu.SemaphoreType.DMA((2 * (2 * COLS + 1),))],
        compiler_params=pltpu.CompilerParams(vmem_limit_bytes=LAYOUT_BYTES),
        name="layout",
    )(fin, loss)
    return (loss.reshape(()), *grads)


def solution(mesh):
    p = _Plan(mesh.shape["dp"])
    rows, vec, whole = P("dp", None), P("dp"), P()
    return jax.shard_map(
        functools.partial(_step, p),
        mesh=mesh,
        in_specs=(rows, rows, vec, vec, whole, whole, whole, whole, whole, whole),
        out_specs=(whole,) * (1 + 2 * COLS),
        check_vma=False,
    )
```
